8 devices in a mesh: dp: 1 (over z), sp: 8 (over y, x, core).
Axes of the slice: x: 2, y: 2, z: 1, core: 2. Of those that a mesh axis runs over, the one named last changes fastest.
Arguments:
- patches: bfloat16 [8192, 1280], P(('dp', 'sp'))
- embeds: bfloat16 [4096, 1536], P(('dp', 'sp'))
- dest_slot: int32 [2048], P(('dp', 'sp'))
- rope_pos: int32 [3, 4096], P(None, ('dp', 'sp'))
- cu_doc: int32 [3], P('dp')
- ln_w: bfloat16 [1280], replicated
- ln_b: bfloat16 [1280], replicated
- w_one: bfloat16 [5120, 5120], replicated
- b_one: bfloat16 [5120], replicated
- w_two: bfloat16 [5120, 1536], replicated
- b_two: bfloat16 [1536], replicated
- norm_attn: bfloat16 [1536], replicated
- w_q: bfloat16 [1536, 1536], replicated
- b_q: bfloat16 [1536], replicated
- w_k: bfloat16 [1536, 256], replicated
- b_k: bfloat16 [256], replicated
- w_v: bfloat16 [1536, 256], replicated
- b_v: bfloat16 [256], replicated
- w_o: bfloat16 [1536, 1536], replicated
- norm_mlp: bfloat16 [1536], replicated
- w_gate: bfloat16 [1536, 8960], replicated
- w_up: bfloat16 [1536, 8960], replicated
- w_down: bfloat16 [8960, 1536], replicated
Outputs:
- output: bfloat16 [4096, 1536], P(('dp', 'sp'))
All inputs are finite; a program needn't handle non-finite values.
Results may differ from the reference program's by a relative error of at most 0.0107451.
Values are sent between devices in bfloat16 or wider.
A program may use at most 1 GiB of HBM per device.

```python
import jax
import jax.numpy as jnp
from jax import lax

GROUP_SIZE = 8
TOK_DEV = 512
MERGED_DEV = 256
HIDDEN = 1536
FFN_DIM = 8960
NUM_HEADS = 12
KV_HEADS = 2
HEAD_DIM = 128
VIT_DIM = 1280
NUM_DOCS = 2

SEQ_LEN = GROUP_SIZE * TOK_DEV
MERGE_DIM = 4 * VIT_DIM
Q_WIDTH = NUM_HEADS * HEAD_DIM
KV_WIDTH = KV_HEADS * HEAD_DIM
NORM_EPS = 1e-6
ROPE_THETA = 1000000.0
MROPE_SPLIT = (16, 40)


def layout_draw(layout_key):
    sub_keys = jax.random.split(layout_key, 7)
    totals = jax.random.randint(sub_keys[0], (GROUP_SIZE,), MERGED_DEV // 4, MERGED_DEV + 1)
    full_dev = jax.random.randint(sub_keys[1], (), 0, GROUP_SIZE)
    totals = jnp.where(jnp.arange(GROUP_SIZE) == full_dev, MERGED_DEV, totals)
    first_len = jax.random.randint(sub_keys[2], (GROUP_SIZE,), 1, totals)
    img_sizes = jnp.stack([first_len, totals - first_len], axis=1).reshape(2 * GROUP_SIZE)
    img_order = jax.random.permutation(sub_keys[3], 2 * GROUP_SIZE)
    text_total = SEQ_LEN - jnp.sum(img_sizes)
    gap_weights = jax.random.randint(sub_keys[4], (2 * GROUP_SIZE + 1,), 1, 17)
    cum_weights = jnp.cumsum(gap_weights)
    text_before = text_total * cum_weights // cum_weights[-1]
    sizes_seq = img_sizes[img_order]
    start_seq = text_before[:-1] + jnp.cumsum(sizes_seq) - sizes_seq
    start_img = jnp.zeros((2 * GROUP_SIZE,), jnp.int32).at[img_order].set(start_seq.astype(jnp.int32))
    row_ids = jnp.arange(GROUP_SIZE * MERGED_DEV)
    dev_of = row_ids // MERGED_DEV
    local_row = row_ids % MERGED_DEV
    first_of = first_len[dev_of]
    second_img = local_row >= first_of
    img_id = 2 * dev_of + second_img.astype(jnp.int32)
    offset = local_row - jnp.where(second_img, first_of, 0)
    dest_slot = jnp.where(local_row < totals[dev_of], start_img[img_id] + offset, -1).astype(jnp.int32)
    doc_cuts = jnp.sort(jax.random.permutation(sub_keys[5], SEQ_LEN - 1)[:NUM_DOCS - 1] + 1).astype(jnp.int32)
    cu_doc = jnp.concatenate([jnp.zeros((1,), jnp.int32), doc_cuts, jnp.full((1,), SEQ_LEN, jnp.int32)])
    tokens = jnp.arange(SEQ_LEN)
    doc_id = jnp.sum(tokens[:, None] >= doc_cuts[None, :], axis=1)
    within = tokens - cu_doc[doc_id]
    is_image = jnp.zeros((SEQ_LEN,), jnp.bool_).at[jnp.where(dest_slot >= 0, dest_slot, SEQ_LEN)].set(True, mode='drop')
    grid_off = jax.random.randint(sub_keys[6], (2, SEQ_LEN), 0, 32)
    rope_pos = jnp.stack([within, within + jnp.where(is_image, grid_off[0], 0), within + jnp.where(is_image, grid_off[1], 0)]).astype(jnp.int32)
    return dest_slot, rope_pos, cu_doc


def gauss_draw(draw_key, shape, scale):
    return jax.random.normal(draw_key, shape, jnp.float32) * scale


def setup_inputs(seed: int = 0, part: int = 0) -> dict:
    root = jax.random.key(seed)
    part_key = jax.random.fold_in(root, part)
    layout_key, patch_key, embed_key = jax.random.split(part_key, 3)
    dest_slot, rope_pos, cu_doc = layout_draw(layout_key)
    wkeys = jax.random.split(jax.random.fold_in(root, 100003), 18)
    bf_type = jnp.bfloat16
    return dict(
        patches=gauss_draw(patch_key, (GROUP_SIZE * 4 * MERGED_DEV, VIT_DIM), 1.0).astype(bf_type),
        embeds=gauss_draw(embed_key, (SEQ_LEN, HIDDEN), 1.0).astype(bf_type),
        dest_slot=dest_slot,
        rope_pos=rope_pos,
        cu_doc=cu_doc,
        ln_w=(1.0 + gauss_draw(wkeys[0], (VIT_DIM,), 0.3)).astype(bf_type),
        ln_b=gauss_draw(wkeys[1], (VIT_DIM,), 0.3).astype(bf_type),
        w_one=gauss_draw(wkeys[2], (MERGE_DIM, MERGE_DIM), MERGE_DIM ** -0.5).astype(bf_type),
        b_one=gauss_draw(wkeys[3], (MERGE_DIM,), 0.5).astype(bf_type),
        w_two=gauss_draw(wkeys[4], (MERGE_DIM, HIDDEN), MERGE_DIM ** -0.5).astype(bf_type),
        b_two=gauss_draw(wkeys[5], (HIDDEN,), 0.5).astype(bf_type),
        norm_attn=(1.0 + gauss_draw(wkeys[6], (HIDDEN,), 0.3)).astype(bf_type),
        w_q=gauss_draw(wkeys[7], (HIDDEN, Q_WIDTH), 1.6 * HIDDEN ** -0.5).astype(bf_type),
        b_q=gauss_draw(wkeys[8], (Q_WIDTH,), 0.5).astype(bf_type),
        w_k=gauss_draw(wkeys[9], (HIDDEN, KV_WIDTH), 1.6 * HIDDEN ** -0.5).astype(bf_type),
        b_k=gauss_draw(wkeys[10], (KV_WIDTH,), 0.5).astype(bf_type),
        w_v=gauss_draw(wkeys[11], (HIDDEN, KV_WIDTH), HIDDEN ** -0.5).astype(bf_type),
        b_v=gauss_draw(wkeys[12], (KV_WIDTH,), 0.5).astype(bf_type),
        w_o=gauss_draw(wkeys[13], (Q_WIDTH, HIDDEN), Q_WIDTH ** -0.5).astype(bf_type),
        norm_mlp=(1.0 + gauss_draw(wkeys[14], (HIDDEN,), 0.3)).astype(bf_type),
        w_gate=gauss_draw(wkeys[15], (HIDDEN, FFN_DIM), HIDDEN ** -0.5).astype(bf_type),
        w_up=gauss_draw(wkeys[16], (HIDDEN, FFN_DIM), HIDDEN ** -0.5).astype(bf_type),
        w_down=gauss_draw(wkeys[17], (FFN_DIM, HIDDEN), FFN_DIM ** -0.5).astype(bf_type),
    )


def layer_norm(values_in, gain_vec, shift_vec):
    widened = values_in.astype(jnp.float32)
    centered = widened - jnp.mean(widened, axis=-1, keepdims=True)
    spread = jnp.mean(centered * centered, axis=-1, keepdims=True)
    return (centered * lax.rsqrt(spread + NORM_EPS) * gain_vec.astype(jnp.float32) + shift_vec.astype(jnp.float32)).astype(jnp.bfloat16)


def rms_norm(values_in, gain_vec):
    widened = values_in.astype(jnp.float32)
    return (widened * lax.rsqrt(jnp.mean(widened * widened, axis=-1, keepdims=True) + NORM_EPS) * gain_vec.astype(jnp.float32)).astype(jnp.bfloat16)


def merger_mlp(grouped, w_one, b_one, w_two, b_two):
    inner = jax.nn.gelu(jnp.dot(grouped, w_one, preferred_element_type=jnp.float32) + b_one.astype(jnp.float32), approximate=False).astype(jnp.bfloat16)
    return (jnp.dot(inner, w_two, preferred_element_type=jnp.float32) + b_two.astype(jnp.float32)).astype(jnp.bfloat16)


def rope_tables(rope_pos):
    inv_freq = ROPE_THETA ** (-jnp.arange(0, HEAD_DIM, 2, dtype=jnp.float32) / HEAD_DIM)
    freq_idx = jnp.arange(HEAD_DIM // 2)[None, :]
    chosen = jnp.where(freq_idx < MROPE_SPLIT[0], rope_pos[0][:, None], jnp.where(freq_idx < MROPE_SPLIT[1], rope_pos[1][:, None], rope_pos[2][:, None]))
    angles = chosen.astype(jnp.float32) * inv_freq[None, :]
    angles = jnp.concatenate([angles, angles], axis=-1)
    return jnp.cos(angles), jnp.sin(angles)


def apply_rope(heads_in, cos_t, sin_t):
    half_dim = HEAD_DIM // 2
    rotated = jnp.concatenate([-heads_in[..., half_dim:], heads_in[..., :half_dim]], axis=-1)
    return heads_in * cos_t[:, None, :] + rotated * sin_t[:, None, :]


def reference(patches, embeds, dest_slot, rope_pos, cu_doc, ln_w, ln_b, w_one, b_one, w_two, b_two, norm_attn, w_q, b_q, w_k, b_k, w_v, b_v, w_o, norm_mlp, w_gate, w_up, w_down):
    normed = layer_norm(patches, ln_w, ln_b).reshape(GROUP_SIZE * MERGED_DEV, MERGE_DIM)
    merged = merger_mlp(normed, w_one, b_one, w_two, b_two)
    target = jnp.where(dest_slot >= 0, dest_slot, SEQ_LEN)
    h_zero = embeds.at[target].set(merged, mode='drop')
    normed_a = rms_norm(h_zero, norm_attn)
    cos_t, sin_t = rope_tables(rope_pos)
    q_lin = jnp.dot(normed_a, w_q, preferred_element_type=jnp.float32) + b_q.astype(jnp.float32)
    k_lin = jnp.dot(normed_a, w_k, preferred_element_type=jnp.float32) + b_k.astype(jnp.float32)
    queries = apply_rope(q_lin.reshape(SEQ_LEN, NUM_HEADS, HEAD_DIM), cos_t, sin_t).astype(jnp.bfloat16)
    keys_rot = apply_rope(k_lin.reshape(SEQ_LEN, KV_HEADS, HEAD_DIM), cos_t, sin_t).astype(jnp.bfloat16)
    values_bf = (jnp.dot(normed_a, w_v, preferred_element_type=jnp.float32) + b_v.astype(jnp.float32)).astype(jnp.bfloat16).reshape(SEQ_LEN, KV_HEADS, HEAD_DIM)
    key_pos = jnp.arange(SEQ_LEN)
    doc_id = jnp.sum(key_pos[:, None] >= cu_doc[None, 1:NUM_DOCS], axis=1)
    keys_wide = keys_rot.astype(jnp.float32)
    values_wide = values_bf.astype(jnp.float32)
    q_blocks = queries.reshape(GROUP_SIZE, TOK_DEV, KV_HEADS, NUM_HEADS // KV_HEADS, HEAD_DIM)

    def attend(block_args):
        block_idx, q_block = block_args
        query_pos = block_idx * TOK_DEV + jnp.arange(TOK_DEV)
        query_doc = lax.dynamic_slice(doc_id, (block_idx * TOK_DEV,), (TOK_DEV,))
        allowed = (key_pos[None, :] <= query_pos[:, None]) & (query_doc[:, None] == doc_id[None, :])
        scores = jnp.einsum('qkgd,tkd->kgqt', q_block.astype(jnp.float32), keys_wide) * HEAD_DIM ** -0.5
        probs_bf = jax.nn.softmax(jnp.where(allowed, scores, -1e30), axis=-1).astype(jnp.bfloat16)
        return jnp.einsum('kgqt,tkd->qkgd', probs_bf.astype(jnp.float32), values_wide).astype(jnp.bfloat16)

    attn_out = lax.map(attend, (jnp.arange(GROUP_SIZE), q_blocks)).reshape(SEQ_LEN, Q_WIDTH)
    h_one = (h_zero.astype(jnp.float32) + jnp.dot(attn_out, w_o, preferred_element_type=jnp.float32)).astype(jnp.bfloat16)
    normed_m = rms_norm(h_one, norm_mlp)
    gate_pre = jnp.dot(normed_m, w_gate, preferred_element_type=jnp.float32)
    up_pre = jnp.dot(normed_m, w_up, preferred_element_type=jnp.float32)
    activated = (jax.nn.silu(gate_pre) * up_pre).astype(jnp.bfloat16)
    return (h_one.astype(jnp.float32) + jnp.dot(activated, w_down, preferred_element_type=jnp.float32)).astype(jnp.bfloat16)
```

```python
import functools
import jax
import jax.numpy as jnp
from jax import lax
from jax.experimental import pallas as pl
from jax.experimental.pallas import tpu as pltpu
from jax.sharding import PartitionSpec as P

BF = jnp.bfloat16
F32 = jnp.float32
MESH=pl.DeviceIdType.MESH
D=128
SC=D**-0.5*1.4426950408889634
def attn_body(n, nh, nkv, cu_ref, q_ref, kt_ref, v_ref, o_ref, qa, kb, vb, acc, mx, ls, ssem, rsem, fsem):
    T=q_ref.shape[0]; grp=nh//nkv
    ncut=cu_ref.shape[0]-2
    me=lax.axis_index('sp'); chip=me//2; core=lax.rem(me,2); partner=chip*2+1-core
    dev=lambda i: {'sp':i}
    bar=pltpu.get_barrier_semaphore()
    for d in range(1,n):
        pl.semaphore_signal(bar,inc=1,device_id=dev(lax.rem(me+d,n)),device_id_type=MESH)
    lane=lax.broadcasted_iota(jnp.int32,(T,D),1); rowq=lax.broadcasted_iota(jnp.int32,(T,D),0)+me*T
    tail=jnp.zeros((T,D),F32)
    for d in range(ncut):
        tail=jnp.where((lane==d)&(rowq>=cu_ref[1+d]),-1e30,tail)
    tail=tail.astype(BF)
    pl.semaphore_wait(bar,n-1)
    def rcopy(what,src_s,g,tgt,sem_s,sem_r,loc=False):
        if what==0:
            src=kt_ref.at[pl.ds(g*D,D),:] if loc else kb.at[src_s,g,pl.ds(0,D),:]
            dst=kb.at[src_s,g,pl.ds(0,D),:]
        else:
            src=v_ref.at[:,pl.ds(g*D,D)] if loc else vb.at[src_s,g]
            dst=vb.at[src_s,g]
        return pltpu.make_async_remote_copy(src_ref=src,dst_ref=dst,send_sem=sem_s,recv_sem=sem_r,device_id=dev(tgt),device_id_type=MESH)
    def my_send(dc,g,w):
        tgt=partner if dc==0 else me+2*dc
        return rcopy(w,me,g,tgt,ssem.at[dc,g,w],rsem.at[me,g,w],loc=True)
    def send_cond(dc):
        return (core==0) if dc==0 else (me+2*dc<n)
    for dc in range(n//2):
        @pl.when(send_cond(dc))
        def _(dc=dc):
            for g in range(nkv):
                for w in range(2): my_send(dc,g,w).start()
    def fill(s,_):
        krow=lax.broadcasted_iota(jnp.int32,(D,T),0); kpos=lax.broadcasted_iota(jnp.int32,(D,T),1)+s*T
        kt=jnp.zeros((D,T),F32)
        for d in range(ncut):
            kt=jnp.where((krow==d)&(kpos<cu_ref[1+d]),1.0,kt)
        kt=kt.astype(BF)
        for g in range(nkv): kb[s,g,pl.ds(D,D),:]=kt
        return 0
    lax.fori_loop(0,n,fill,0)
    for h in range(nh):
        qa[h,:,:D]=q_ref[:,h*D:(h+1)*D]
        qa[h,:,D:]=tail
    for g in range(nkv):
        kb[me,g,pl.ds(0,D),:]=kt_ref[g*D:(g+1)*D,:]
    HB=T//2
    def own(h,_):
        g=h//grp
        for r in range(2):
            rows=pl.ds(r*HB,HB); W=(r+1)*HB
            s=jnp.dot(qa[h,rows,:],kb[me,g,:,pl.ds(0,W)],preferred_element_type=F32)*SC
            qi=lax.broadcasted_iota(jnp.int32,(HB,W),0)+r*HB; ki=lax.broadcasted_iota(jnp.int32,(HB,W),1)
            s=jnp.where(ki<=qi,s,-1e30)
            m=jnp.max(s,axis=1,keepdims=True)
            p=jnp.exp2(s-m)
            l=p[:,:D]
            for j in range(1,W//D): l=l+p[:,j*D:(j+1)*D]
            mx[h,rows,:]=jnp.broadcast_to(m,(HB,D)); ls[h,rows,:]=l
            vg=v_ref[pl.ds(0,W),pl.ds(pl.multiple_of(g*D,D),D)]
            acc[h,rows,:]=jnp.dot(p.astype(BF),vg,preferred_element_type=F32)
        return 0
    lax.fori_loop(0,nh,own,0)
    def head_step(h,s,g):
        sc=jnp.dot(qa[h],kb[s,g],preferred_element_type=F32)*SC
        mp=mx[h]
        m=jnp.maximum(mp,jnp.max(sc,axis=1,keepdims=True))
        al=jnp.exp2(mp-m)
        l=ls[h]*al; ps=[]
        for j in range(T//D):
            p=jnp.exp2(sc[:,j*D:(j+1)*D]-m); l=l+p; ps.append(p.astype(BF))
        p=jnp.concatenate(ps,axis=1)
        mx[h]=m; ls[h]=l
        acc[h]=acc[h]*al+jnp.dot(p,vb[s,g],preferred_element_type=F32)
    def wait_recv(s,g):
        for w in range(2): rcopy(w,s,g,partner,fsem.at[0,g,w],rsem.at[s,g,w]).wait_recv()
    def fwd(s,g,w,dc): return rcopy(w,s,g,partner,fsem.at[dc,g,w],rsem.at[s,g,w])
    def shard_step(i,_):
        j=i-core
        dc=jnp.where(j<0,0,j//2+1)
        direct=(j>=0)&(lax.rem(j+2,2)==0)
        s=jnp.where(j<0,partner,(chip-dc)*2+jnp.where(direct,core,1-core))
        for g in range(nkv):
            wait_recv(s,g)
            @pl.when(direct)
            def _():
                for w in range(2): fwd(s,g,w,dc).start()
            for hh in range(grp): head_step(g*grp+hh,s,g)
        return 0
    lax.fori_loop(0,2*chip+core,shard_step,0)
    for h in range(nh):
        o_ref[:,h*D:(h+1)*D]=(acc[h]/jnp.sum(ls[h],axis=1,keepdims=True)).astype(BF)
    for dc in range(n//2):
        @pl.when(send_cond(dc))
        def _(dc=dc):
            for g in range(nkv):
                for w in range(2): my_send(dc,g,w).wait_send()
    for dc in range(1,n//2):
        @pl.when(chip-dc>=0)
        def _(dc=dc):
            s=(chip-dc)*2+core
            for g in range(nkv):
                for w in range(2): fwd(s,g,w,dc).wait_send()
def attn_call(cu,q,kt,v,n=8):
    T,HQ=q.shape; nh=HQ//D; nkv=kt.shape[0]//D
    vm=pl.BlockSpec(memory_space=pltpu.VMEM)
    return pl.pallas_call(functools.partial(attn_body,n,nh,nkv),
        out_shape=jax.ShapeDtypeStruct((T,HQ),BF),
        in_specs=[pl.BlockSpec(memory_space=pltpu.SMEM),vm,vm,vm],
        out_specs=vm,
        scratch_shapes=[pltpu.VMEM((nh,T,2*D),BF),pltpu.VMEM((n,nkv,2*D,T),BF),pltpu.VMEM((n,nkv,T,D),BF),
            pltpu.VMEM((nh,T,D),F32),pltpu.VMEM((nh,T,D),F32),pltpu.VMEM((nh,T,D),F32),
            pltpu.SemaphoreType.DMA((n//2,nkv,2)),pltpu.SemaphoreType.DMA((n,nkv,2)),pltpu.SemaphoreType.DMA((n//2,nkv,2))],
        compiler_params=pltpu.CompilerParams(collective_id=1,has_side_effects=True,vmem_limit_bytes=56*1024*1024),
        cost_estimate=pl.CostEstimate(flops=4*T*T*n*HQ,bytes_accessed=4*T*HQ,transcendentals=T*T*n*nh),
        name="attn")(cu,q,kt,v)

def mlp_body(nsub, h0_ref, at_ref, wo_ref, nm_ref, wg_ref, wu_ref, wd_ref, out_ref, b_scr, acc_scr):
    i=pl.program_id(0)
    @pl.when(i==0)
    def _():
        for r in range(2):
            rows=pl.ds(r*256,256)
            h1=(h0_ref[rows,:].astype(F32)+jnp.dot(at_ref[rows,:],wo_ref[...],preferred_element_type=F32)).astype(BF)
            h1w=h1.astype(F32)
            acc_scr[rows,:]=h1w
            b_scr[rows,:]=(h1w*lax.rsqrt(jnp.mean(h1w*h1w,axis=-1,keepdims=True)+1e-6)*nm_ref[...].astype(F32)).astype(BF)
    b=b_scr[...]
    tf=wg_ref.shape[1]; sub=tf//nsub
    acts=[]
    for j in range(nsub):
        cols=slice(j*sub,(j+1)*sub)
        g=jnp.dot(b,wg_ref[:,cols],preferred_element_type=F32)
        u=jnp.dot(b,wu_ref[:,cols],preferred_element_type=F32)
        acts.append((g*jax.nn.sigmoid(g)*u).astype(BF))
    a=jnp.concatenate(acts,axis=1) if nsub>1 else acts[0]
    acc_scr[...]+=jnp.dot(a,wd_ref[...],preferred_element_type=F32)
    @pl.when(i==pl.num_programs(0)-1)
    def _():
        out_ref[...]=acc_scr[...].astype(BF)
def mlp_call(h0,at,wo,nm,wg,wu,wd,tf=1280,nsub=5):
    T,H=h0.shape; Fd=wg.shape[1]
    full=lambda s: pl.BlockSpec(s,lambda i:(0,)*len(s),pipeline_mode=pl.Buffered(1))
    return pl.pallas_call(functools.partial(mlp_body,nsub),
        out_shape=jax.ShapeDtypeStruct((T,H),BF),
        grid=(Fd//tf,),
        in_specs=[full((T,H)),full((T,H)),full((H,H)),full((1,H)),
                  pl.BlockSpec((H,tf),lambda i:(0,i)),pl.BlockSpec((H,tf),lambda i:(0,i)),pl.BlockSpec((tf,H),lambda i:(i,0))],
        out_specs=pl.BlockSpec((T,H),lambda i:(0,0),pipeline_mode=pl.Buffered(1)),
        scratch_shapes=[pltpu.VMEM((T,H),BF),pltpu.VMEM((T,H),F32)],
        compiler_params=pltpu.CompilerParams(dimension_semantics=("arbitrary",),vmem_limit_bytes=60*1024*1024),
        cost_estimate=pl.CostEstimate(flops=2*T*H*(H+3*Fd),bytes_accessed=2*H*(H+3*Fd),transcendentals=T*Fd),
        name="mlp",
    )(h0,at,wo,nm.reshape(1,H),wg,wu,wd)

HEAD_DIM = 128
NORM_EPS = 1e-6
ROPE_THETA = 1000000.0
MROPE_SPLIT = (16, 40)


def layer_norm(values_in, gain_vec, shift_vec):
    widened = values_in.astype(jnp.float32)
    centered = widened - jnp.mean(widened, axis=-1, keepdims=True)
    spread = jnp.mean(centered * centered, axis=-1, keepdims=True)
    return (centered * lax.rsqrt(spread + NORM_EPS) * gain_vec.astype(jnp.float32) + shift_vec.astype(jnp.float32)).astype(jnp.bfloat16)


def rms_norm(values_in, gain_vec):
    widened = values_in.astype(jnp.float32)
    return (widened * lax.rsqrt(jnp.mean(widened * widened, axis=-1, keepdims=True) + NORM_EPS) * gain_vec.astype(jnp.float32)).astype(jnp.bfloat16)


def merger_mlp(grouped, w_one, b_one, w_two, b_two):
    inner = jax.nn.gelu(jnp.dot(grouped, w_one, preferred_element_type=jnp.float32) + b_one.astype(jnp.float32), approximate=False).astype(jnp.bfloat16)
    return (jnp.dot(inner, w_two, preferred_element_type=jnp.float32) + b_two.astype(jnp.float32)).astype(jnp.bfloat16)


def rope_tables(rope_pos):
    inv_freq = ROPE_THETA ** (-jnp.arange(0, HEAD_DIM, 2, dtype=jnp.float32) / HEAD_DIM)
    freq_idx = jnp.arange(HEAD_DIM // 2)[None, :]
    chosen = jnp.where(freq_idx < MROPE_SPLIT[0], rope_pos[0][:, None], jnp.where(freq_idx < MROPE_SPLIT[1], rope_pos[1][:, None], rope_pos[2][:, None]))
    angles = chosen.astype(jnp.float32) * inv_freq[None, :]
    angles = jnp.concatenate([angles, angles], axis=-1)
    return jnp.cos(angles), jnp.sin(angles)


def apply_rope(heads_in, cos_t, sin_t):
    half_dim = HEAD_DIM // 2
    rotated = jnp.concatenate([-heads_in[..., half_dim:], heads_in[..., :half_dim]], axis=-1)
    return heads_in * cos_t[:, None, :] + rotated * sin_t[:, None, :]


def qkv_project(normed_a, rope_pos, w_q, b_q, w_k, b_k, w_v, b_v):
    tokens = normed_a.shape[0]
    cos_t, sin_t = rope_tables(rope_pos)
    q_lin = jnp.dot(normed_a, w_q, preferred_element_type=jnp.float32) + b_q.astype(jnp.float32)
    k_lin = jnp.dot(normed_a, w_k, preferred_element_type=jnp.float32) + b_k.astype(jnp.float32)
    queries = apply_rope(q_lin.reshape(tokens, -1, HEAD_DIM), cos_t, sin_t).astype(jnp.bfloat16)
    keys_rot = apply_rope(k_lin.reshape(tokens, -1, HEAD_DIM), cos_t, sin_t).astype(jnp.bfloat16)
    values_bf = (jnp.dot(normed_a, w_v, preferred_element_type=jnp.float32) + b_v.astype(jnp.float32)).astype(jnp.bfloat16).reshape(tokens, -1, HEAD_DIM)
    return queries, keys_rot, values_bf


def solution(mesh):
    group_size = mesh.shape['sp']
    row_spec = P(('dp', 'sp'), None)

    def local_step(patches, embeds, dest_slot, rope_pos, cu_doc, ln_w, ln_b, w_one, b_one, w_two, b_two, norm_attn, w_q, b_q, w_k, b_k, w_v, b_v, w_o, norm_mlp, w_gate, w_up, w_down):
        tok_dev = embeds.shape[0]
        merged_dev = dest_slot.shape[0]
        my_shard = lax.axis_index('sp')
        normed = layer_norm(patches, ln_w, ln_b).reshape(merged_dev, -1)
        merged = merger_mlp(normed, w_one, b_one, w_two, b_two)
        to_shard = dest_slot // tok_dev
        send_mask = to_shard[None, :] == jnp.arange(group_size)[:, None]
        send_buf = jnp.where(send_mask[:, :, None], merged[None, :, :], 0)
        received = lax.all_to_all(send_buf, 'sp', 0, 0, tiled=True).reshape(group_size * merged_dev, -1)
        all_slots = lax.all_gather(dest_slot, 'sp', tiled=True)
        pick_mask = all_slots[None, :] == (my_shard * tok_dev + jnp.arange(tok_dev))[:, None]
        placed = jnp.dot(pick_mask.astype(jnp.bfloat16), received, preferred_element_type=jnp.float32).astype(jnp.bfloat16)
        h_zero = jnp.where(jnp.any(pick_mask, axis=1)[:, None], placed, embeds)
        queries, keys_loc, values_loc = qkv_project(rms_norm(h_zero, norm_attn), rope_pos, w_q, b_q, w_k, b_k, w_v, b_v)
        kt_loc = keys_loc.reshape(tok_dev, -1).T
        attn_out = attn_call(cu_doc, queries.reshape(tok_dev, -1), kt_loc, values_loc.reshape(tok_dev, -1), group_size)
        return mlp_call(h_zero, attn_out, w_o, norm_mlp, w_gate, w_up, w_down)

    in_specs = (row_spec, row_spec, P(('dp', 'sp')), P(None, ('dp', 'sp')), P('dp')) + (P(),) * 18
    return jax.shard_map(local_step, mesh=mesh, in_specs=in_specs, out_specs=row_spec, check_vma=False)
```

```python
import functools
import jax
import jax.numpy as jnp
from jax import lax
from jax.experimental import pallas as pl
from jax.experimental.pallas import tpu as pltpu
from jax.sharding import PartitionSpec as P

BF = jnp.bfloat16
F32 = jnp.float32
MESH = pl.DeviceIdType.MESH
D = 128
SC=D**-0.5*1.4426950408889634
def attn_body(n, nh, nkv, cu_ref, q_ref, kt_ref, v_ref, o_ref, qa, kb, vb, acc, mx, ls, ssem, rsem, fsem):
    T=q_ref.shape[0]; grp=nh//nkv
    ncut=cu_ref.shape[0]-2
    me=lax.axis_index('sp'); chip=me//2; core=lax.rem(me,2); partner=chip*2+1-core
    dev=lambda i: {'sp':i}
    bar=pltpu.get_barrier_semaphore()
    for d in range(1,n):
        pl.semaphore_signal(bar,inc=1,device_id=dev(lax.rem(me+d,n)),device_id_type=MESH)
    lane=lax.broadcasted_iota(jnp.int32,(T,D),1); rowq=lax.broadcasted_iota(jnp.int32,(T,D),0)+me*T
    tail=jnp.zeros((T,D),F32)
    for d in range(ncut):
        tail=jnp.where((lane==d)&(rowq>=cu_ref[1+d]),-1e30,tail)
    tail=tail.astype(BF)
    pl.semaphore_wait(bar,n-1)
    def rcopy(what,src_s,g,tgt,sem_s,sem_r,loc=False):
        if what==0:
            src=kt_ref.at[pl.ds(g*D,D),:] if loc else kb.at[src_s,g,pl.ds(0,D),:]
            dst=kb.at[src_s,g,pl.ds(0,D),:]
        else:
            src=v_ref.at[:,pl.ds(g*D,D)] if loc else vb.at[src_s,g]
            dst=vb.at[src_s,g]
        return pltpu.make_async_remote_copy(src_ref=src,dst_ref=dst,send_sem=sem_s,recv_sem=sem_r,device_id=dev(tgt),device_id_type=MESH)
    def my_send(dc,g,w):
        tgt=partner if dc==0 else me+2*dc
        return rcopy(w,me,g,tgt,ssem.at[dc,g,w],rsem.at[me,g,w],loc=True)
    def send_cond(dc):
        return (core==0) if dc==0 else (me+2*dc<n)
    for dc in range(n//2):
        @pl.when(send_cond(dc))
        def _(dc=dc):
            for g in range(nkv):
                for w in range(2): my_send(dc,g,w).start()
    def fill(s,_):
        krow=lax.broadcasted_iota(jnp.int32,(D,T),0); kpos=lax.broadcasted_iota(jnp.int32,(D,T),1)+s*T
        kt=jnp.zeros((D,T),F32)
        for d in range(ncut):
            kt=jnp.where((krow==d)&(kpos<cu_ref[1+d]),1.0,kt)
        kt=kt.astype(BF)
        for g in range(nkv): kb[s,g,pl.ds(D,D),:]=kt
        return 0
    lax.fori_loop(0,n,fill,0)
    for h in range(nh):
        qa[h,:,:D]=q_ref[:,h*D:(h+1)*D]
        qa[h,:,D:]=tail
    for g in range(nkv):
        kb[me,g,pl.ds(0,D),:]=kt_ref[g*D:(g+1)*D,:]
    HB=T//2
    def own(h,_):
        g=h//grp
        for r in range(2):
            rows=pl.ds(r*HB,HB); W=(r+1)*HB
            s=jnp.dot(qa[h,rows,:],kb[me,g,:,pl.ds(0,W)],preferred_element_type=F32)*SC
            qi=lax.broadcasted_iota(jnp.int32,(HB,W),0)+r*HB; ki=lax.broadcasted_iota(jnp.int32,(HB,W),1)
            s=jnp.where(ki<=qi,s,-1e30)
            m=jnp.max(s,axis=1,keepdims=True)
            p=jnp.exp2(s-m)
            l=p[:,:D]
            for j in range(1,W//D): l=l+p[:,j*D:(j+1)*D]
            mx[h,rows,:]=jnp.broadcast_to(m,(HB,D)); ls[h,rows,:]=l
            vg=v_ref[pl.ds(0,W),pl.ds(pl.multiple_of(g*D,D),D)]
            acc[h,rows,:]=jnp.dot(p.astype(BF),vg,preferred_element_type=F32)
        return 0
    lax.fori_loop(0,nh,own,0)
    def head_step(h,s,g):
        sc=jnp.dot(qa[h],kb[s,g],preferred_element_type=F32)*SC
        mp=mx[h]
        m=jnp.maximum(mp,jnp.max(sc,axis=1,keepdims=True))
        al=jnp.exp2(mp-m)
        l=ls[h]*al; ps=[]
        for j in range(T//D):
            p=jnp.exp2(sc[:,j*D:(j+1)*D]-m); l=l+p; ps.append(p.astype(BF))
        p=jnp.concatenate(ps,axis=1)
        mx[h]=m; ls[h]=l
        acc[h]=acc[h]*al+jnp.dot(p,vb[s,g],preferred_element_type=F32)
    def wait_recv(s,g):
        for w in range(2): rcopy(w,s,g,partner,fsem.at[0,g,w],rsem.at[s,g,w]).wait_recv()
    def fwd(s,g,w,dc): return rcopy(w,s,g,partner,fsem.at[dc,g,w],rsem.at[s,g,w])
    def shard_step(i,_):
        j=i-core
        dc=jnp.where(j<0,0,j//2+1)
        direct=(j>=0)&(lax.rem(j+2,2)==0)
        s=jnp.where(j<0,partner,(chip-dc)*2+jnp.where(direct,core,1-core))
        for g in range(nkv):
            wait_recv(s,g)
            @pl.when(direct)
            def _():
                for w in range(2): fwd(s,g,w,dc).start()
            for hh in range(grp): head_step(g*grp+hh,s,g)
        return 0
    lax.fori_loop(0,2*chip+core,shard_step,0)
    for h in range(nh):
        o_ref[:,h*D:(h+1)*D]=(acc[h]/jnp.sum(ls[h],axis=1,keepdims=True)).astype(BF)
    for dc in range(n//2):
        @pl.when(send_cond(dc))
        def _(dc=dc):
            for g in range(nkv):
                for w in range(2): my_send(dc,g,w).wait_send()
    for dc in range(1,n//2):
        @pl.when(chip-dc>=0)
        def _(dc=dc):
            s=(chip-dc)*2+core
            for g in range(nkv):
                for w in range(2): fwd(s,g,w,dc).wait_send()
def attn_call(cu,q,kt,v,n=8):
    T,HQ=q.shape; nh=HQ//D; nkv=kt.shape[0]//D
    vm=pl.BlockSpec(memory_space=pltpu.VMEM)
    return pl.pallas_call(functools.partial(attn_body,n,nh,nkv),
        out_shape=jax.ShapeDtypeStruct((T,HQ),BF),
        in_specs=[pl.BlockSpec(memory_space=pltpu.SMEM),vm,vm,vm],
        out_specs=vm,
        scratch_shapes=[pltpu.VMEM((nh,T,2*D),BF),pltpu.VMEM((n,nkv,2*D,T),BF),pltpu.VMEM((n,nkv,T,D),BF),
            pltpu.VMEM((nh,T,D),F32),pltpu.VMEM((nh,T,D),F32),pltpu.VMEM((nh,T,D),F32),
            pltpu.SemaphoreType.DMA((n//2,nkv,2)),pltpu.SemaphoreType.DMA((n,nkv,2)),pltpu.SemaphoreType.DMA((n//2,nkv,2))],
        compiler_params=pltpu.CompilerParams(collective_id=1,has_side_effects=True,vmem_limit_bytes=56*1024*1024),
        cost_estimate=pl.CostEstimate(flops=4*T*T*n*HQ,bytes_accessed=4*T*HQ,transcendentals=T*T*n*nh),
        name="attn")(cu,q,kt,v)
TW=256
NB=5
def front_body(n, pat_ref, emb_ref, slot_ref, cos_ref, sin_ref, lw_ref, lb_ref, w1_ref, b1_ref, w2_ref, b2_ref, na_ref, wq_ref, bq_ref, wk_ref, bk_ref, wv_ref, bv_ref,
               h0_ref, q_ref, kt_ref, v_ref,
               zf, z, inner, wbuf, mbuf, slots, onehot, hacc, wq, wk, wv,
               wsem, qsem, slot_s, slot_r, own_s, fwd_s, rsem):
    R=mbuf.shape[1]; T=emb_ref.shape[0]; V=pat_ref.shape[1]; K1=w1_ref.shape[0]; H=w2_ref.shape[1]
    n1=w1_ref.shape[1]//TW; n2=H//TW
    me=lax.axis_index('sp'); chip=me//2; core=lax.rem(me,2)
    partner=chip*2+1-core
    cx=lax.rem(chip,2); cy=chip//2
    xn=(cy*2+1-cx)*2+core; yn=((1-cy)*2+cx)*2+core; dg=((1-cy)*2+1-cx)*2+core
    other=lambda i: i+1-2*core
    dev=lambda i: {'sp':i}
    bar=pltpu.get_barrier_semaphore()
    for d in range(1,n):
        pl.semaphore_signal(bar,inc=1,device_id=dev(lax.rem(me+d,n)),device_id_type=MESH)
    def w1copy(t,s): return pltpu.make_async_copy(w1_ref.at[:,pl.ds(pl.multiple_of(t*TW,TW),TW)],wbuf.at[s],wsem.at[s])
    def w2copy(t,s): return pltpu.make_async_copy(w2_ref.at[:,pl.ds(pl.multiple_of(t*TW,TW),TW)],wbuf.at[s],wsem.at[s])
    for t in range(NB): w1copy(t,t).start()
    CH=128
    def ln(i,_):
        x=pat_ref[pl.ds(pl.multiple_of(i*CH,CH),CH),:].astype(F32)
        c=x-jnp.mean(x,axis=-1,keepdims=True)
        var=jnp.mean(c*c,axis=-1,keepdims=True)
        y=c*lax.rsqrt(var+1e-6)*lw_ref[...].astype(F32)+lb_ref[...].astype(F32)
        for p in range(V//D): zf[p]=y[:,p*D:(p+1)*D]
        for j in range(4):
            for p in range(V//D):
                z[pl.ds(pl.multiple_of(i*(CH//4),CH//4),CH//4),j*V+p*D:j*V+(p+1)*D]=zf[p,pl.ds(j,CH//4,stride=4),:].astype(BF)
        return 0
    lax.fori_loop(0,pat_ref.shape[0]//CH,ln,0)
    pl.semaphore_wait(bar,n-1)
    def slot_copy(d):
        return pltpu.make_async_remote_copy(src_ref=slot_ref,dst_ref=slots.at[me],send_sem=slot_s.at[d-1],recv_sem=slot_r.at[me],device_id=dev(lax.rem(me+d,n)),device_id_type=MESH)
    for d in range(1,n): slot_copy(d).start()
    slots[me]=slot_ref[...]
    def first(i,_):
        s=lax.rem(i,NB)
        w1copy(i,s).wait()
        y=jnp.dot(z[...],wbuf[s],preferred_element_type=F32)
        cols=pl.ds(pl.multiple_of(i*TW,TW),TW)
        y=y+b1_ref[:,cols].astype(F32)
        inner[:,cols]=(0.5*y*(1.0+lax.erf(y*0.7071067811865476))).astype(BF)
        @pl.when(i+NB<n1)
        def _(): w1copy(i+NB,s).start()
        @pl.when(i+NB>=n1)
        def _(): w2copy(i+NB-n1,s).start()
        return 0
    lax.fori_loop(0,n1,first,0)
    qc=pltpu.make_async_copy(wq_ref,wq,qsem.at[0]); kc=pltpu.make_async_copy(wk_ref,wk,qsem.at[1]); vc=pltpu.make_async_copy(wv_ref,wv,qsem.at[2])
    def tile(s,j): return mbuf.at[s,:,pl.ds(j*TW,TW)]
    def send(src,j,tgt,ss):
        return pltpu.make_async_remote_copy(src_ref=tile(src,j),dst_ref=tile(src,j),send_sem=ss,recv_sem=rsem.at[src,j],device_id=dev(tgt),device_id_type=MESH)
    for j in range(n2):
        t=n1+j; s=t%NB
        w2copy(j,s).wait()
        y=jnp.dot(inner[...],wbuf[s],preferred_element_type=F32)+b2_ref[:,j*TW:(j+1)*TW].astype(F32)
        mbuf[me,:,j*TW:(j+1)*TW]=y.astype(BF)
        for a,tgt in enumerate((xn,yn,partner)): send(me,j,tgt,own_s.at[a,j]).start()
        if t+NB<n1+n2: w2copy(j+NB,s).start()
        elif t+NB==n1+n2: qc.start(); kc.start(); vc.start()
    for d in range(1,n):
        s=lax.rem(me+d,n)
        pltpu.make_async_remote_copy(src_ref=slot_ref,dst_ref=slots.at[s],send_sem=slot_s.at[0],recv_sem=slot_r.at[s],device_id=dev(s),device_id_type=MESH).wait_recv()
    base=me*T
    def oh(s,_):
        sl=slots[s][0:1,:]
        tok=lax.broadcasted_iota(jnp.int32,(T,R),0)+base
        onehot[s]=jnp.where(tok==sl,1.0,0.0).astype(BF)
        return 0
    lax.fori_loop(0,n,oh,0)
    def place(s,j,firsttime=False):
        c=slice(j*TW,(j+1)*TW)
        p=jnp.dot(onehot[s],mbuf[s,:,c],preferred_element_type=F32)
        if firsttime: hacc[:,c]=p
        else: hacc[:,c]+=p
    for j in range(n2): place(me,j,True)
    def arrive(s,j): send(s,j,partner,own_s.at[0,0]).wait_recv()
    fw=[]
    def forward(s,j,tgt,kind):
        c=send(s,j,tgt,fwd_s.at[kind,j]); c.start(); fw.append(c)
    for j in range(n2):
        arrive(xn,j)
        if j%2==0: forward(xn,j,yn,0)
        forward(xn,j,partner,1)
        arrive(yn,j)
        if j%2==1: forward(yn,j,xn,0)
        forward(yn,j,partner,2)
        arrive(partner,j)
        place(xn,j); place(yn,j); place(partner,j)
        if j>0:
            for s in (other(xn),other(yn)):
                arrive(s,j-1); place(s,j-1)
    for s in (other(xn),other(yn)):
        arrive(s,n2-1); place(s,n2-1)
    for j in range(n2):
        arrive(dg,j); forward(dg,j,partner,3); place(dg,j)
        if j>0: arrive(other(dg),j-1); place(other(dg),j-1)
    arrive(other(dg),n2-1); place(other(dg),n2-1)
    hit=onehot[0].astype(F32)
    for s in range(1,n): hit=hit+onehot[s].astype(F32)
    has=jnp.sum(hit,axis=1,keepdims=True)>0.5
    h0=jnp.where(has,hacc[...],emb_ref[...].astype(F32))
    h0_ref[...]=h0.astype(BF)
    a=(h0*lax.rsqrt(jnp.mean(h0*h0,axis=-1,keepdims=True)+1e-6)*na_ref[...].astype(F32)).astype(BF)
    qc.wait(); kc.wait(); vc.wait()
    def rope(x):
        return x*cos_ref[...]+pltpu.roll(x,D//2,1)*sin_ref[...]
    for i in range(H//TW):
        y=jnp.dot(a,wq[:,i*TW:(i+1)*TW],preferred_element_type=F32)+bq_ref[:,i*TW:(i+1)*TW].astype(F32)
        for h in range(TW//D):
            q_ref[:,i*TW+h*D:i*TW+(h+1)*D]=rope(y[:,h*D:(h+1)*D]).astype(BF)
    y=jnp.dot(a,wk[...],preferred_element_type=F32)+bk_ref[...].astype(F32)
    for h in range(wk.shape[1]//D):
        kt_ref[h*D:(h+1)*D,:]=rope(y[:,h*D:(h+1)*D]).T.astype(BF)
    v_ref[...]=(jnp.dot(a,wv[...],preferred_element_type=F32)+bv_ref[...].astype(F32)).astype(BF)
    for d in range(1,n): slot_copy(d).wait_send()
    for j in range(n2):
        for a_,tgt in enumerate((xn,yn,partner)): send(me,j,tgt,own_s.at[a_,j]).wait_send()
    for c in fw: c.wait_send()
def rope_tables(rope_pos):
    inv_freq = 1000000.0 ** (-jnp.arange(0, 128, 2, dtype=jnp.float32) / 128)
    fi = jnp.arange(64)[None, :]
    chosen = jnp.where(fi < 16, rope_pos[0][:, None], jnp.where(fi < 40, rope_pos[1][:, None], rope_pos[2][:, None]))
    ang = chosen.astype(jnp.float32) * inv_freq[None, :]
    c, s = jnp.cos(ang), jnp.sin(ang)
    return jnp.concatenate([c, c], axis=-1), jnp.concatenate([-s, s], axis=-1)
def front_call(pat,emb,slot,rope_pos,lw,lb,w1,b1,w2,b2,na,wq,bq,wk,bk,wv,bv,n=8):
    T,H=emb.shape; R=slot.shape[0]; K1=w1.shape[0]; V=pat.shape[1]; KV=wk.shape[1]
    cos,sin=rope_tables(rope_pos)
    slot8=jnp.broadcast_to(slot[None,:],(8,R))
    vm=pl.BlockSpec(memory_space=pltpu.VMEM); hbm=pl.BlockSpec(memory_space=pl.ANY)
    r1=lambda x: x.reshape(1,-1)
    n2=H//TW
    DS=pltpu.SemaphoreType.DMA
    return pl.pallas_call(functools.partial(front_body,n),
        out_shape=(jax.ShapeDtypeStruct((T,H),BF),jax.ShapeDtypeStruct((T,wq.shape[1]),BF),jax.ShapeDtypeStruct((KV,T),BF),jax.ShapeDtypeStruct((T,KV),BF)),
        in_specs=[vm,vm,vm,vm,vm,vm,vm,hbm,vm,hbm,vm,vm,hbm,vm,hbm,vm,hbm,vm],
        out_specs=(vm,)*4,
        scratch_shapes=[pltpu.VMEM((V//D,128,D),F32),pltpu.VMEM((R,K1),BF),pltpu.VMEM((R,w1.shape[1]),BF),pltpu.VMEM((NB,K1,TW),BF),
            pltpu.VMEM((n,R,H),BF),pltpu.VMEM((n,8,R),jnp.int32),pltpu.VMEM((n,T,R),BF),pltpu.VMEM((T,H),F32),
            pltpu.VMEM(wq.shape,BF),pltpu.VMEM(wk.shape,BF),pltpu.VMEM(wv.shape,BF),
            DS((NB,)),DS((3,)),DS((n-1,)),DS((n,)),DS((3,n2)),DS((4,n2)),DS((n,n2))],
        compiler_params=pltpu.CompilerParams(collective_id=2,has_side_effects=True,vmem_limit_bytes=62*1024*1024),
        cost_estimate=pl.CostEstimate(flops=2*R*K1*(K1+H),bytes_accessed=2*K1*(K1+H),transcendentals=R*K1),
        name="front")(pat,emb,slot8,cos,sin,r1(lw),r1(lb),w1,r1(b1),w2,r1(b2),r1(na),wq,r1(bq),wk,r1(bk),wv,r1(bv))
def mlp_body(nsub, h0_ref, at_ref, wo_ref, nm_ref, wg_ref, wu_ref, wd_ref, out_ref, b_scr, acc_scr):
    i=pl.program_id(0)
    @pl.when(i==0)
    def _():
        for r in range(2):
            rows=pl.ds(r*256,256)
            h1=(h0_ref[rows,:].astype(F32)+jnp.dot(at_ref[rows,:],wo_ref[...],preferred_element_type=F32)).astype(BF)
            h1w=h1.astype(F32)
            acc_scr[rows,:]=h1w
            b_scr[rows,:]=(h1w*lax.rsqrt(jnp.mean(h1w*h1w,axis=-1,keepdims=True)+1e-6)*nm_ref[...].astype(F32)).astype(BF)
    b=b_scr[...]
    tf=wg_ref.shape[1]; sub=tf//nsub
    acts=[]
    for j in range(nsub):
        cols=slice(j*sub,(j+1)*sub)
        g=jnp.dot(b,wg_ref[:,cols],preferred_element_type=F32)
        u=jnp.dot(b,wu_ref[:,cols],preferred_element_type=F32)
        acts.append((g*jax.nn.sigmoid(g)*u).astype(BF))
    a=jnp.concatenate(acts,axis=1) if nsub>1 else acts[0]
    acc_scr[...]+=jnp.dot(a,wd_ref[...],preferred_element_type=F32)
    @pl.when(i==pl.num_programs(0)-1)
    def _():
        out_ref[...]=acc_scr[...].astype(BF)
def mlp_call(h0,at,wo,nm,wg,wu,wd,tf=1280,nsub=5):
    T,H=h0.shape; Fd=wg.shape[1]
    full=lambda s: pl.BlockSpec(s,lambda i:(0,)*len(s),pipeline_mode=pl.Buffered(1))
    return pl.pallas_call(functools.partial(mlp_body,nsub),
        out_shape=jax.ShapeDtypeStruct((T,H),BF),
        grid=(Fd//tf,),
        in_specs=[full((T,H)),full((T,H)),full((H,H)),full((1,H)),
                  pl.BlockSpec((H,tf),lambda i:(0,i)),pl.BlockSpec((H,tf),lambda i:(0,i)),pl.BlockSpec((tf,H),lambda i:(i,0))],
        out_specs=pl.BlockSpec((T,H),lambda i:(0,0),pipeline_mode=pl.Buffered(1)),
        scratch_shapes=[pltpu.VMEM((T,H),BF),pltpu.VMEM((T,H),F32)],
        compiler_params=pltpu.CompilerParams(dimension_semantics=("arbitrary",),vmem_limit_bytes=60*1024*1024),
        cost_estimate=pl.CostEstimate(flops=2*T*H*(H+3*Fd),bytes_accessed=2*H*(H+3*Fd),transcendentals=T*Fd),
        name="mlp",
    )(h0,at,wo,nm.reshape(1,H),wg,wu,wd)


def solution(mesh):
    group_size = mesh.shape['sp']
    row_spec = P(('dp', 'sp'), None)

    def local_step(patches, embeds, dest_slot, rope_pos, cu_doc, ln_w, ln_b, w_one, b_one, w_two, b_two, norm_attn, w_q, b_q, w_k, b_k, w_v, b_v, w_o, norm_mlp, w_gate, w_up, w_down):
        h_zero, q, k, v = front_call(patches, embeds, dest_slot, rope_pos, ln_w, ln_b, w_one, b_one, w_two, b_two, norm_attn, w_q, b_q, w_k, b_k, w_v, b_v, group_size)
        attn_out = attn_call(cu_doc, q, k, v, group_size)
        return mlp_call(h_zero, attn_out, w_o, norm_mlp, w_gate, w_up, w_down)

    in_specs = (row_spec, row_spec, P(('dp', 'sp')), P(None, ('dp', 'sp')), P('dp')) + (P(),) * 18
    return jax.shard_map(local_step, mesh=mesh, in_specs=in_specs, out_specs=row_spec, check_vma=False)
```

```python
import functools
import jax
import jax.numpy as jnp
from jax import lax
from jax.experimental import pallas as pl
from jax.experimental.pallas import tpu as pltpu
from jax.sharding import PartitionSpec as P

BF = jnp.bfloat16
F32 = jnp.float32
MESH = pl.DeviceIdType.MESH
D = 128
SC=D**-0.5*1.4426950408889634
def attn_body(n, nh, nkv, cu_ref, q_ref, kt_ref, v_ref, o_ref, qa, kb, vb, acc, mx, ls, sb, pb, ssem, rsem, fsem):
    T=q_ref.shape[0]; grp=nh//nkv
    ncut=cu_ref.shape[0]-2
    me=lax.axis_index('sp'); chip=me//2; core=lax.rem(me,2); partner=chip*2+1-core
    dev=lambda i: {'sp':i}
    bar=pltpu.get_barrier_semaphore()
    for d in range(1,n):
        pl.semaphore_signal(bar,inc=1,device_id=dev(lax.rem(me+d,n)),device_id_type=MESH)
    lane=lax.broadcasted_iota(jnp.int32,(T,D),1); rowq=lax.broadcasted_iota(jnp.int32,(T,D),0)+me*T
    tail=jnp.zeros((T,D),F32)
    for d in range(ncut):
        tail=jnp.where((lane==d)&(rowq>=cu_ref[1+d]),-1e30,tail)
    tail=tail.astype(BF)
    pl.semaphore_wait(bar,n-1)
    def rcopy(what,src_s,g,tgt,sem_s,sem_r,loc=False):
        if what==0:
            src=kt_ref.at[pl.ds(g*D,D),:] if loc else kb.at[src_s,g,pl.ds(0,D),:]
            dst=kb.at[src_s,g,pl.ds(0,D),:]
        else:
            src=v_ref.at[:,pl.ds(g*D,D)] if loc else vb.at[src_s,g]
            dst=vb.at[src_s,g]
        return pltpu.make_async_remote_copy(src_ref=src,dst_ref=dst,send_sem=sem_s,recv_sem=sem_r,device_id=dev(tgt),device_id_type=MESH)
    def my_send(dc,g,w):
        tgt=partner if dc==0 else me+2*dc
        return rcopy(w,me,g,tgt,ssem.at[dc,g,w],rsem.at[me,g,w],loc=True)
    def send_cond(dc):
        return (core==0) if dc==0 else (me+2*dc<n)
    for dc in range(n//2):
        @pl.when(send_cond(dc))
        def _(dc=dc):
            for g in range(nkv):
                for w in range(2): my_send(dc,g,w).start()
    def fill(s,_):
        krow=lax.broadcasted_iota(jnp.int32,(D,T),0); kpos=lax.broadcasted_iota(jnp.int32,(D,T),1)+s*T
        kt=jnp.zeros((D,T),F32)
        for d in range(ncut):
            kt=jnp.where((krow==d)&(kpos<cu_ref[1+d]),1.0,kt)
        kt=kt.astype(BF)
        for g in range(nkv): kb[s,g,pl.ds(D,D),:]=kt
        return 0
    lax.fori_loop(0,n,fill,0)
    for h in range(nh):
        qa[h,:,:D]=q_ref[:,h*D:(h+1)*D]
        qa[h,:,D:]=tail
    for g in range(nkv):
        kb[me,g,pl.ds(0,D),:]=kt_ref[g*D:(g+1)*D,:]
    HB=T//2
    def own(h,_):
        g=h//grp
        for r in range(2):
            rows=pl.ds(r*HB,HB); W=(r+1)*HB
            s=jnp.dot(qa[h,rows,:],kb[me,g,:,pl.ds(0,W)],preferred_element_type=F32)*SC
            qi=lax.broadcasted_iota(jnp.int32,(HB,W),0)+r*HB; ki=lax.broadcasted_iota(jnp.int32,(HB,W),1)
            s=jnp.where(ki<=qi,s,-1e30)
            m=jnp.max(s,axis=1,keepdims=True)
            p=jnp.exp2(s-m)
            l=p[:,:D]
            for j in range(1,W//D): l=l+p[:,j*D:(j+1)*D]
            mx[h,rows,:]=jnp.broadcast_to(m,(HB,D)); ls[h,rows,:]=l
            vg=v_ref[pl.ds(0,W),pl.ds(pl.multiple_of(g*D,D),D)]
            acc[h,rows,:]=jnp.dot(p.astype(BF),vg,preferred_element_type=F32)
        return 0
    lax.fori_loop(0,nh,own,0)
    def qk(h,s,g): return jnp.dot(qa[h],kb[s,g],preferred_element_type=F32)
    def soft(h,sc):
        mp=mx[h]
        m=jnp.maximum(mp,jnp.max(sc,axis=1,keepdims=True)*SC)
        al=jnp.exp2(mp-m)
        l=ls[h]*al; ps=[]
        for j in range(T//D):
            p=jnp.exp2(sc[:,j*D:(j+1)*D]*SC-m); l=l+p; ps.append(p.astype(BF))
        mx[h]=m; ls[h]=l
        return jnp.concatenate(ps,axis=1),al
    def pv(h,s,g,p,al):
        acc[h]=acc[h]*al+jnp.dot(p,vb[s,g],preferred_element_type=F32)
    def wait_recv(s,g):
        for w in range(2): rcopy(w,s,g,partner,fsem.at[0,g,w],rsem.at[s,g,w]).wait_recv()
    def fwd(s,g,w,dc): return rcopy(w,s,g,partner,fsem.at[dc,g,w],rsem.at[s,g,w])
    def shard_step(i,_):
        j=i-core
        dc=jnp.where(j<0,0,j//2+1)
        direct=(j>=0)&(lax.rem(j+2,2)==0)
        s=jnp.where(j<0,partner,(chip-dc)*2+jnp.where(direct,core,1-core))
        for g in range(nkv):
            wait_recv(s,g)
            @pl.when(direct)
            def _():
                for w in range(2): fwd(s,g,w,dc).start()
            sb[0]=qk(g*grp,s,g)
            for hh in range(grp):
                h=g*grp+hh
                if hh+1<grp: sb[(hh+1)%2]=qk(h+1,s,g)
                if hh>0: pv(h-1,s,g,pb[(hh-1)%2],albuf)
                p,albuf=soft(h,sb[hh%2])
                pb[hh%2]=p
            pv(g*grp+grp-1,s,g,pb[(grp-1)%2],albuf)
        return 0
    lax.fori_loop(0,2*chip+core,shard_step,0)
    for h in range(nh):
        o_ref[:,h*D:(h+1)*D]=(acc[h]/jnp.sum(ls[h],axis=1,keepdims=True)).astype(BF)
    for dc in range(n//2):
        @pl.when(send_cond(dc))
        def _(dc=dc):
            for g in range(nkv):
                for w in range(2): my_send(dc,g,w).wait_send()
    for dc in range(1,n//2):
        @pl.when(chip-dc>=0)
        def _(dc=dc):
            s=(chip-dc)*2+core
            for g in range(nkv):
                for w in range(2): fwd(s,g,w,dc).wait_send()
def attn_call(cu,q,kt,v,n=8):
    T,HQ=q.shape; nh=HQ//D; nkv=kt.shape[0]//D
    vm=pl.BlockSpec(memory_space=pltpu.VMEM)
    return pl.pallas_call(functools.partial(attn_body,n,nh,nkv),
        out_shape=jax.ShapeDtypeStruct((T,HQ),BF),
        in_specs=[pl.BlockSpec(memory_space=pltpu.SMEM),vm,vm,vm],
        out_specs=vm,
        scratch_shapes=[pltpu.VMEM((nh,T,2*D),BF),pltpu.VMEM((n,nkv,2*D,T),BF),pltpu.VMEM((n,nkv,T,D),BF),
            pltpu.VMEM((nh,T,D),F32),pltpu.VMEM((nh,T,D),F32),pltpu.VMEM((nh,T,D),F32),
            pltpu.VMEM((2,T,T),F32),pltpu.VMEM((2,T,T),BF),
            pltpu.SemaphoreType.DMA((n//2,nkv,2)),pltpu.SemaphoreType.DMA((n,nkv,2)),pltpu.SemaphoreType.DMA((n//2,nkv,2))],
        compiler_params=pltpu.CompilerParams(collective_id=1,has_side_effects=True,vmem_limit_bytes=56*1024*1024),
        cost_estimate=pl.CostEstimate(flops=4*T*T*n*HQ,bytes_accessed=4*T*HQ,transcendentals=T*T*n*nh),
        name="attn")(cu,q,kt,v)
TW=256
NB=5
def front_body(n, pat_ref, emb_ref, slot_ref, rp_ref, lw_ref, lb_ref, w1_ref, b1_ref, w2_ref, b2_ref, na_ref, wq_ref, bq_ref, wk_ref, bk_ref, wv_ref, bv_ref,
               h0_ref, q_ref, kt_ref, v_ref,
               zf, z, inner, wbuf, mbuf, slots, onehot, hacc, wq, wk, wv,
               cs, sn, wsem, qsem, slot_s, slot_r, own_s, fwd_s, rsem):
    R=mbuf.shape[1]; T=emb_ref.shape[0]; V=pat_ref.shape[1]; K1=w1_ref.shape[0]; H=w2_ref.shape[1]
    n1=w1_ref.shape[1]//TW; n2=H//TW
    me=lax.axis_index('sp'); chip=me//2; core=lax.rem(me,2)
    partner=chip*2+1-core
    cx=lax.rem(chip,2); cy=chip//2
    xn=(cy*2+1-cx)*2+core; yn=((1-cy)*2+cx)*2+core; dg=((1-cy)*2+1-cx)*2+core
    other=lambda i: i+1-2*core
    dev=lambda i: {'sp':i}
    bar=pltpu.get_barrier_semaphore()
    for d in range(1,n):
        pl.semaphore_signal(bar,inc=1,device_id=dev(lax.rem(me+d,n)),device_id_type=MESH)
    def w1copy(t,s): return pltpu.make_async_copy(w1_ref.at[:,pl.ds(pl.multiple_of(t*TW,TW),TW)],wbuf.at[s],wsem.at[s])
    def w2copy(t,s): return pltpu.make_async_copy(w2_ref.at[:,pl.ds(pl.multiple_of(t*TW,TW),TW)],wbuf.at[s],wsem.at[s])
    for t in range(NB): w1copy(t,t).start()
    slots[me]=jnp.broadcast_to(slot_ref[...].reshape(1,R),(8,R))
    lw=lw_ref[...].astype(F32).reshape(1,V); lb=lb_ref[...].astype(F32).reshape(1,V)
    CH=128
    def ln(i,_):
        x=pat_ref[pl.ds(pl.multiple_of(i*CH,CH),CH),:].astype(F32)
        c=x-jnp.mean(x,axis=-1,keepdims=True)
        var=jnp.mean(c*c,axis=-1,keepdims=True)
        y=c*lax.rsqrt(var+1e-6)*lw+lb
        for p in range(V//D): zf[p]=y[:,p*D:(p+1)*D]
        for j in range(4):
            for p in range(V//D):
                z[pl.ds(pl.multiple_of(i*(CH//4),CH//4),CH//4),j*V+p*D:j*V+(p+1)*D]=zf[p,pl.ds(j,CH//4,stride=4),:].astype(BF)
        return 0
    lax.fori_loop(0,pat_ref.shape[0]//CH,ln,0)
    pl.semaphore_wait(bar,n-1)
    def slot_copy(d):
        return pltpu.make_async_remote_copy(src_ref=slots.at[me],dst_ref=slots.at[me],send_sem=slot_s.at[d-1],recv_sem=slot_r.at[me],device_id=dev(lax.rem(me+d,n)),device_id_type=MESH)
    for d in range(1,n): slot_copy(d).start()
    def first(i,_):
        s=lax.rem(i,NB)
        w1copy(i,s).wait()
        y=jnp.dot(z[...],wbuf[s],preferred_element_type=F32)
        cols=pl.ds(pl.multiple_of(i*TW,TW),TW)
        y=y+b1_ref[cols].astype(F32).reshape(1,TW)
        inner[:,cols]=(0.5*y*(1.0+lax.erf(y*0.7071067811865476))).astype(BF)
        @pl.when(i+NB<n1)
        def _(): w1copy(i+NB,s).start()
        @pl.when(i+NB>=n1)
        def _(): w2copy(i+NB-n1,s).start()
        return 0
    lax.fori_loop(0,n1,first,0)
    qc=pltpu.make_async_copy(wq_ref,wq,qsem.at[0]); kc=pltpu.make_async_copy(wk_ref,wk,qsem.at[1]); vc=pltpu.make_async_copy(wv_ref,wv,qsem.at[2])
    def tile(s,j): return mbuf.at[s,:,pl.ds(j*TW,TW)]
    def send(src,j,tgt,ss):
        return pltpu.make_async_remote_copy(src_ref=tile(src,j),dst_ref=tile(src,j),send_sem=ss,recv_sem=rsem.at[src,j],device_id=dev(tgt),device_id_type=MESH)
    for j in range(n2):
        t=n1+j; s=t%NB
        w2copy(j,s).wait()
        y=jnp.dot(inner[...],wbuf[s],preferred_element_type=F32)+b2_ref[j*TW:(j+1)*TW].astype(F32).reshape(1,TW)
        mbuf[me,:,j*TW:(j+1)*TW]=y.astype(BF)
        for a,tgt in enumerate((xn,yn,partner)): send(me,j,tgt,own_s.at[a,j]).start()
        if t+NB<n1+n2: w2copy(j+NB,s).start()
        elif t+NB==n1+n2: qc.start(); kc.start(); vc.start()
    for d in range(1,n):
        s=lax.rem(me+d,n)
        pltpu.make_async_remote_copy(src_ref=slots.at[s],dst_ref=slots.at[s],send_sem=slot_s.at[0],recv_sem=slot_r.at[s],device_id=dev(s),device_id_type=MESH).wait_recv()
    base=me*T
    def oh(s,_):
        sl=slots[s][0:1,:]
        tok=lax.broadcasted_iota(jnp.int32,(T,R),0)+base
        onehot[s]=jnp.where(tok==sl,1.0,0.0).astype(BF)
        return 0
    lax.fori_loop(0,n,oh,0)
    def place(s,j,firsttime=False):
        c=slice(j*TW,(j+1)*TW)
        p=jnp.dot(onehot[s],mbuf[s,:,c],preferred_element_type=F32)
        if firsttime: hacc[:,c]=p
        else: hacc[:,c]+=p
    for j in range(n2): place(me,j,True)
    fi=lax.broadcasted_iota(jnp.int32,(D//2,T),0)
    pos=jnp.where(fi<16,rp_ref[0:1,:],jnp.where(fi<40,rp_ref[1:2,:],rp_ref[2:3,:]))
    fr=jnp.zeros((D//2,D),F32); fj=lax.broadcasted_iota(jnp.int32,(D//2,D),0)
    for i in range(D//2): fr=jnp.where(fj==i,1000000.0**(-i/(D//2)),fr)
    ang=pos.astype(F32)*fr[:,0:1]
    cc=jnp.cos(ang); ss=jnp.sin(ang)
    cs[...]=jnp.concatenate([cc,cc],axis=0).T
    sn[...]=jnp.concatenate([-ss,ss],axis=0).T
    def arrive(s,j): send(s,j,partner,own_s.at[0,0]).wait_recv()
    fw=[]
    def forward(s,j,tgt,kind):
        c=send(s,j,tgt,fwd_s.at[kind,j]); c.start(); fw.append(c)
    for j in range(n2):
        arrive(xn,j)
        if j%2==0: forward(xn,j,yn,0)
        forward(xn,j,partner,1)
        arrive(yn,j)
        if j%2==1: forward(yn,j,xn,0)
        forward(yn,j,partner,2)
        arrive(partner,j)
        place(xn,j); place(yn,j); place(partner,j)
        if j>0:
            for s in (other(xn),other(yn)):
                arrive(s,j-1); place(s,j-1)
    for s in (other(xn),other(yn)):
        arrive(s,n2-1); place(s,n2-1)
    for j in range(n2):
        arrive(dg,j); forward(dg,j,partner,3); place(dg,j)
        if j>0: arrive(other(dg),j-1); place(other(dg),j-1)
    arrive(other(dg),n2-1); place(other(dg),n2-1)
    hit=onehot[0].astype(F32)
    for s in range(1,n): hit=hit+onehot[s].astype(F32)
    has=jnp.sum(hit,axis=1,keepdims=True)>0.5
    h0=jnp.where(has,hacc[...],emb_ref[...].astype(F32))
    h0_ref[...]=h0.astype(BF)
    a=(h0*lax.rsqrt(jnp.mean(h0*h0,axis=-1,keepdims=True)+1e-6)*na_ref[...].astype(F32).reshape(1,H)).astype(BF)
    qc.wait(); kc.wait(); vc.wait()
    def rope(x):
        return x*cs[...]+pltpu.roll(x,D//2,1)*sn[...]
    for i in range(H//TW):
        y=jnp.dot(a,wq[:,i*TW:(i+1)*TW],preferred_element_type=F32)+bq_ref[i*TW:(i+1)*TW].astype(F32).reshape(1,TW)
        for h in range(TW//D):
            q_ref[:,i*TW+h*D:i*TW+(h+1)*D]=rope(y[:,h*D:(h+1)*D]).astype(BF)
    y=jnp.dot(a,wk[...],preferred_element_type=F32)+bk_ref[...].astype(F32).reshape(1,-1)
    for h in range(wk.shape[1]//D):
        kt_ref[h*D:(h+1)*D,:]=rope(y[:,h*D:(h+1)*D]).T.astype(BF)
    v_ref[...]=(jnp.dot(a,wv[...],preferred_element_type=F32)+bv_ref[...].astype(F32).reshape(1,-1)).astype(BF)
    for d in range(1,n): slot_copy(d).wait_send()
    for j in range(n2):
        for a_,tgt in enumerate((xn,yn,partner)): send(me,j,tgt,own_s.at[a_,j]).wait_send()
    for c in fw: c.wait_send()
def front_call(pat,emb,slot,rope_pos,lw,lb,w1,b1,w2,b2,na,wq,bq,wk,bk,wv,bv,n=8):
    T,H=emb.shape; R=slot.shape[0]; K1=w1.shape[0]; V=pat.shape[1]; KV=wk.shape[1]
    vm=pl.BlockSpec(memory_space=pltpu.VMEM); hbm=pl.BlockSpec(memory_space=pl.ANY)
    n2=H//TW
    DS=pltpu.SemaphoreType.DMA
    return pl.pallas_call(functools.partial(front_body,n),
        out_shape=(jax.ShapeDtypeStruct((T,H),BF),jax.ShapeDtypeStruct((T,wq.shape[1]),BF),jax.ShapeDtypeStruct((KV,T),BF),jax.ShapeDtypeStruct((T,KV),BF)),
        in_specs=[vm,vm,vm,vm,vm,vm,hbm,vm,hbm,vm,vm,hbm,vm,hbm,vm,hbm,vm],
        out_specs=(vm,)*4,
        scratch_shapes=[pltpu.VMEM((V//D,128,D),F32),pltpu.VMEM((R,K1),BF),pltpu.VMEM((R,w1.shape[1]),BF),pltpu.VMEM((NB,K1,TW),BF),
            pltpu.VMEM((n,R,H),BF),pltpu.VMEM((n,8,R),jnp.int32),pltpu.VMEM((n,T,R),BF),pltpu.VMEM((T,H),F32),
            pltpu.VMEM(wq.shape,BF),pltpu.VMEM(wk.shape,BF),pltpu.VMEM(wv.shape,BF),pltpu.VMEM((T,D),F32),pltpu.VMEM((T,D),F32),
            DS((NB,)),DS((3,)),DS((n-1,)),DS((n,)),DS((3,n2)),DS((4,n2)),DS((n,n2))],
        compiler_params=pltpu.CompilerParams(collective_id=2,has_side_effects=True,vmem_limit_bytes=62*1024*1024),
        cost_estimate=pl.CostEstimate(flops=2*R*K1*(K1+H),bytes_accessed=2*K1*(K1+H),transcendentals=R*K1),
        name="front")(pat,emb,slot,rope_pos,lw,lb,w1,b1,w2,b2,na,wq,bq,wk,bk,wv,bv)
def mlp_body(nsub, h0_ref, at_ref, wo_ref, nm_ref, wg_ref, wu_ref, wd_ref, out_ref, b_scr, acc_scr):
    i=pl.program_id(0)
    @pl.when(i==0)
    def _():
        for r in range(2):
            rows=pl.ds(r*256,256)
            h1=(h0_ref[rows,:].astype(F32)+jnp.dot(at_ref[rows,:],wo_ref[...],preferred_element_type=F32)).astype(BF)
            h1w=h1.astype(F32)
            acc_scr[rows,:]=h1w
            b_scr[rows,:]=(h1w*lax.rsqrt(jnp.mean(h1w*h1w,axis=-1,keepdims=True)+1e-6)*nm_ref[...].astype(F32).reshape(1,-1)).astype(BF)
    b=b_scr[...]
    tf=wg_ref.shape[1]; sub=tf//nsub
    acts=[]
    for j in range(nsub):
        cols=slice(j*sub,(j+1)*sub)
        g=jnp.dot(b,wg_ref[:,cols],preferred_element_type=F32)
        u=jnp.dot(b,wu_ref[:,cols],preferred_element_type=F32)
        acts.append((g*jax.nn.sigmoid(g)*u).astype(BF))
    a=jnp.concatenate(acts,axis=1) if nsub>1 else acts[0]
    acc_scr[...]+=jnp.dot(a,wd_ref[...],preferred_element_type=F32)
    @pl.when(i==pl.num_programs(0)-1)
    def _():
        out_ref[...]=acc_scr[...].astype(BF)
def mlp_call(h0,at,wo,nm,wg,wu,wd,tf=1280,nsub=5):
    T,H=h0.shape; Fd=wg.shape[1]
    full=lambda s: pl.BlockSpec(s,lambda i:(0,)*len(s),pipeline_mode=pl.Buffered(1))
    return pl.pallas_call(functools.partial(mlp_body,nsub),
        out_shape=jax.ShapeDtypeStruct((T,H),BF),
        grid=(Fd//tf,),
        in_specs=[full((T,H)),full((T,H)),full((H,H)),pl.BlockSpec(memory_space=pltpu.VMEM),
                  pl.BlockSpec((H,tf),lambda i:(0,i)),pl.BlockSpec((H,tf),lambda i:(0,i)),pl.BlockSpec((tf,H),lambda i:(i,0))],
        out_specs=pl.BlockSpec((T,H),lambda i:(0,0),pipeline_mode=pl.Buffered(1)),
        scratch_shapes=[pltpu.VMEM((T,H),BF),pltpu.VMEM((T,H),F32)],
        compiler_params=pltpu.CompilerParams(dimension_semantics=("arbitrary",),vmem_limit_bytes=60*1024*1024),
        cost_estimate=pl.CostEstimate(flops=2*T*H*(H+3*Fd),bytes_accessed=2*H*(H+3*Fd),transcendentals=T*Fd),
        name="mlp",
    )(h0,at,wo,nm,wg,wu,wd)


def solution(mesh):
    group_size = mesh.shape['sp']
    row_spec = P(('dp', 'sp'), None)

    def local_step(patches, embeds, dest_slot, rope_pos, cu_doc, ln_w, ln_b, w_one, b_one, w_two, b_two, norm_attn, w_q, b_q, w_k, b_k, w_v, b_v, w_o, norm_mlp, w_gate, w_up, w_down):
        h_zero, q, k, v = front_call(patches, embeds, dest_slot, rope_pos, ln_w, ln_b, w_one, b_one, w_two, b_two, norm_attn, w_q, b_q, w_k, b_k, w_v, b_v, group_size)
        attn_out = attn_call(cu_doc, q, k, v, group_size)
        return mlp_call(h_zero, attn_out, w_o, norm_mlp, w_gate, w_up, w_down)

    in_specs = (row_spec, row_spec, P(('dp', 'sp')), P(None, ('dp', 'sp')), P('dp')) + (P(),) * 18
    return jax.shard_map(local_step, mesh=mesh, in_specs=in_specs, out_specs=row_spec, check_vma=False)
```

```python
import functools
import jax
import jax.numpy as jnp
from jax import lax
from jax.experimental import pallas as pl
from jax.experimental.pallas import tpu as pltpu
from jax.sharding import PartitionSpec as P

BF = jnp.bfloat16
F32 = jnp.float32
MESH = pl.DeviceIdType.MESH
D = 128
SC=D**-0.5*1.4426950408889634
def attn_body(n, nh, nkv, cu_ref, q_ref, kt_ref, v_ref, o_ref, qa, kb, vb, acc, mx, ls, sb, pb, ssem, rsem, fsem):
    T=q_ref.shape[0]; grp=nh//nkv
    ncut=cu_ref.shape[0]-2
    me=lax.axis_index('sp'); chip=me//2; core=lax.rem(me,2); partner=chip*2+1-core
    dev=lambda i: {'sp':i}
    bar=pltpu.get_barrier_semaphore()
    for d in range(1,n):
        pl.semaphore_signal(bar,inc=1,device_id=dev(lax.rem(me+d,n)),device_id_type=MESH)
    lane=lax.broadcasted_iota(jnp.int32,(T,D),1); rowq=lax.broadcasted_iota(jnp.int32,(T,D),0)+me*T
    tail=jnp.zeros((T,D),F32)
    for d in range(ncut):
        tail=jnp.where((lane==d)&(rowq>=cu_ref[1+d]),-1e30,tail)
    tail=tail.astype(BF)
    pl.semaphore_wait(bar,n-1)
    def rcopy(what,src_s,g,tgt,sem_s,sem_r,loc=False):
        if what==0:
            src=kt_ref.at[pl.ds(g*D,D),:] if loc else kb.at[src_s,g,pl.ds(0,D),:]
            dst=kb.at[src_s,g,pl.ds(0,D),:]
        else:
            src=v_ref.at[:,pl.ds(g*D,D)] if loc else vb.at[src_s,g]
            dst=vb.at[src_s,g]
        return pltpu.make_async_remote_copy(src_ref=src,dst_ref=dst,send_sem=sem_s,recv_sem=sem_r,device_id=dev(tgt),device_id_type=MESH)
    def my_send(dc,g,w):
        tgt=partner if dc==0 else me+2*dc
        return rcopy(w,me,g,tgt,ssem.at[dc,g,w],rsem.at[me,g,w],loc=True)
    def send_cond(dc):
        return (core==0) if dc==0 else (me+2*dc<n)
    for dc in range(n//2):
        @pl.when(send_cond(dc))
        def _(dc=dc):
            for g in range(nkv):
                for w in range(2): my_send(dc,g,w).start()
    def fill(s,_):
        krow=lax.broadcasted_iota(jnp.int32,(D,T),0); kpos=lax.broadcasted_iota(jnp.int32,(D,T),1)+s*T
        kt=jnp.zeros((D,T),F32)
        for d in range(ncut):
            kt=jnp.where((krow==d)&(kpos<cu_ref[1+d]),1.0,kt)
        kt=kt.astype(BF)
        for g in range(nkv): kb[s,g,pl.ds(D,D),:]=kt
        return 0
    lax.fori_loop(0,me+1,fill,0)
    for h in range(nh):
        qa[h,:,:D]=q_ref[:,h*D:(h+1)*D]
        qa[h,:,D:]=tail
    for g in range(nkv):
        kb[me,g,pl.ds(0,D),:]=kt_ref[g*D:(g+1)*D,:]
        vb[me,g]=v_ref[:,g*D:(g+1)*D]
    def qk(h,s,g): return jnp.dot(qa[h],kb[s,g],preferred_element_type=F32)
    def soft(h,sc):
        mp=mx[h]
        m=jnp.maximum(mp,jnp.max(sc,axis=1,keepdims=True)*SC)
        al=jnp.exp2(mp-m)
        l=ls[h]*al; ps=[]
        for j in range(T//D):
            p=jnp.exp2(sc[:,j*D:(j+1)*D]*SC-m); l=l+p; ps.append(p.astype(BF))
        mx[h]=m; ls[h]=l
        return jnp.concatenate(ps,axis=1),al
    def pv(h,s,g,p,al):
        acc[h]=acc[h]*al+jnp.dot(p,vb[s,g],preferred_element_type=F32)
    def soft_own(h,sc):
        qi=lax.broadcasted_iota(jnp.int32,(T,T),0); ki=lax.broadcasted_iota(jnp.int32,(T,T),1)
        sc=jnp.where(ki<=qi,sc,-1e30)
        m=jnp.broadcast_to(jnp.max(sc,axis=1,keepdims=True)*SC,(T,D))
        l=None; ps=[]
        for j in range(T//D):
            p=jnp.exp2(sc[:,j*D:(j+1)*D]*SC-m); l=p if l is None else l+p
            ps.append(p.astype(BF))
        mx[h]=m; ls[h]=l
        return jnp.concatenate(ps,axis=1)
    def pv_own(h,g,p): acc[h]=jnp.dot(p,vb[me,g],preferred_element_type=F32)
    def own(g,_):
        h0=g*grp
        sb[0]=qk(h0,me,g)
        for hh in range(grp):
            h=h0+hh
            if hh+1<grp: sb[(hh+1)%2]=qk(h+1,me,g)
            if hh>0: pv_own(h-1,g,pb[(hh-1)%2])
            pb[hh%2]=soft_own(h,sb[hh%2])
        pv_own(h0+grp-1,g,pb[(grp-1)%2])
        return 0
    lax.fori_loop(0,nkv,own,0)
    def wait_recv(s,g):
        for w in range(2): rcopy(w,s,g,partner,fsem.at[0,g,w],rsem.at[s,g,w]).wait_recv()
    def fwd(s,g,w,dc): return rcopy(w,s,g,partner,fsem.at[dc,g,w],rsem.at[s,g,w])
    def shard_step(i,_):
        j=i-core
        dc=jnp.where(j<0,0,j//2+1)
        direct=(j>=0)&(lax.rem(j+2,2)==0)
        s=jnp.where(j<0,partner,(chip-dc)*2+jnp.where(direct,core,1-core))
        def per_g(g,_):
            wait_recv(s,g)
            @pl.when(direct)
            def _():
                for w in range(2): fwd(s,g,w,dc).start()
            sb[0]=qk(g*grp,s,g)
            for hh in range(grp):
                h=g*grp+hh
                if hh+1<grp: sb[(hh+1)%2]=qk(h+1,s,g)
                if hh>0: pv(h-1,s,g,pb[(hh-1)%2],albuf)
                p,albuf=soft(h,sb[hh%2])
                pb[hh%2]=p
            pv(g*grp+grp-1,s,g,pb[(grp-1)%2],albuf)
            return 0
        lax.fori_loop(0,nkv,per_g,0)
        return 0
    lax.fori_loop(0,2*chip+core,shard_step,0)
    for h in range(nh):
        o_ref[:,h*D:(h+1)*D]=(acc[h]/jnp.sum(ls[h],axis=1,keepdims=True)).astype(BF)
    for dc in range(n//2):
        @pl.when(send_cond(dc))
        def _(dc=dc):
            for g in range(nkv):
                for w in range(2): my_send(dc,g,w).wait_send()
    for dc in range(1,n//2):
        @pl.when(chip-dc>=0)
        def _(dc=dc):
            s=(chip-dc)*2+core
            for g in range(nkv):
                for w in range(2): fwd(s,g,w,dc).wait_send()
def attn_call(cu,q,kt,v,n=8):
    T,HQ=q.shape; nh=HQ//D; nkv=kt.shape[0]//D
    vm=pl.BlockSpec(memory_space=pltpu.VMEM)
    return pl.pallas_call(functools.partial(attn_body,n,nh,nkv),
        out_shape=jax.ShapeDtypeStruct((T,HQ),BF),
        in_specs=[pl.BlockSpec(memory_space=pltpu.SMEM),vm,vm,vm],
        out_specs=vm,
        scratch_shapes=[pltpu.VMEM((nh,T,2*D),BF),pltpu.VMEM((n,nkv,2*D,T),BF),pltpu.VMEM((n,nkv,T,D),BF),
            pltpu.VMEM((nh,T,D),F32),pltpu.VMEM((nh,T,D),F32),pltpu.VMEM((nh,T,D),F32),
            pltpu.VMEM((2,T,T),F32),pltpu.VMEM((2,T,T),BF),
            pltpu.SemaphoreType.DMA((n//2,nkv,2)),pltpu.SemaphoreType.DMA((n,nkv,2)),pltpu.SemaphoreType.DMA((n//2,nkv,2))],
        compiler_params=pltpu.CompilerParams(collective_id=1,has_side_effects=True,vmem_limit_bytes=56*1024*1024),
        cost_estimate=pl.CostEstimate(flops=4*T*T*n*HQ,bytes_accessed=4*T*HQ,transcendentals=T*T*n*nh),
        name="attn")(cu,q,kt,v)
TW=256
NB=5
def front_body(n, pat_ref, emb_ref, slot_ref, rp_ref, lw_ref, lb_ref, w1_ref, b1_ref, w2_ref, b2_ref, na_ref, wq_ref, bq_ref, wk_ref, bk_ref, wv_ref, bv_ref,
               h0_ref, q_ref, kt_ref, v_ref,
               zf, z, inner, wbuf, mbuf, slots, onehot, hacc, wq, wk, wv,
               cs, sn, wsem, qsem, slot_s, slot_r, own_s, fwd_s, rsem):
    R=mbuf.shape[1]; T=emb_ref.shape[0]; V=pat_ref.shape[1]; K1=w1_ref.shape[0]; H=w2_ref.shape[1]
    n1=w1_ref.shape[1]//TW; n2=H//TW
    me=lax.axis_index('sp'); chip=me//2; core=lax.rem(me,2)
    partner=chip*2+1-core
    cx=lax.rem(chip,2); cy=chip//2
    xn=(cy*2+1-cx)*2+core; yn=((1-cy)*2+cx)*2+core; dg=((1-cy)*2+1-cx)*2+core
    other=lambda i: i+1-2*core
    dev=lambda i: {'sp':i}
    bar=pltpu.get_barrier_semaphore()
    for d in range(1,n):
        pl.semaphore_signal(bar,inc=1,device_id=dev(lax.rem(me+d,n)),device_id_type=MESH)
    def w1copy(t,s): return pltpu.make_async_copy(w1_ref.at[:,pl.ds(pl.multiple_of(t*TW,TW),TW)],wbuf.at[s],wsem.at[s])
    def w2copy(t,s): return pltpu.make_async_copy(w2_ref.at[:,pl.ds(pl.multiple_of(t*TW,TW),TW)],wbuf.at[s],wsem.at[s])
    for t in range(NB): w1copy(t,t).start()
    slots[me]=jnp.broadcast_to(slot_ref[...].reshape(1,R),(8,R))
    lw=lw_ref[...].astype(F32).reshape(1,V); lb=lb_ref[...].astype(F32).reshape(1,V)
    CH=128
    def ln(i,_):
        x=pat_ref[pl.ds(pl.multiple_of(i*CH,CH),CH),:].astype(F32)
        c=x-jnp.mean(x,axis=-1,keepdims=True)
        var=jnp.mean(c*c,axis=-1,keepdims=True)
        y=c*lax.rsqrt(var+1e-6)*lw+lb
        for p in range(V//D): zf[p]=y[:,p*D:(p+1)*D]
        for j in range(4):
            for p in range(V//D):
                z[pl.ds(pl.multiple_of(i*(CH//4),CH//4),CH//4),j*V+p*D:j*V+(p+1)*D]=zf[p,pl.ds(j,CH//4,stride=4),:].astype(BF)
        return 0
    lax.fori_loop(0,pat_ref.shape[0]//CH,ln,0)
    pl.semaphore_wait(bar,n-1)
    def slot_copy(d):
        return pltpu.make_async_remote_copy(src_ref=slots.at[me],dst_ref=slots.at[me],send_sem=slot_s.at[d-1],recv_sem=slot_r.at[me],device_id=dev(lax.rem(me+d,n)),device_id_type=MESH)
    for d in range(1,n): slot_copy(d).start()
    def first(i,_):
        s=lax.rem(i,NB)
        w1copy(i,s).wait()
        y=jnp.dot(z[...],wbuf[s],preferred_element_type=F32)
        cols=pl.ds(pl.multiple_of(i*TW,TW),TW)
        y=y+b1_ref[cols].astype(F32).reshape(1,TW)
        inner[:,cols]=(0.5*y*(1.0+lax.erf(y*0.7071067811865476))).astype(BF)
        @pl.when(i+NB<n1)
        def _(): w1copy(i+NB,s).start()
        @pl.when(i+NB>=n1)
        def _(): w2copy(i+NB-n1,s).start()
        return 0
    lax.fori_loop(0,n1,first,0)
    qc=pltpu.make_async_copy(wq_ref,wq,qsem.at[0]); kc=pltpu.make_async_copy(wk_ref,wk,qsem.at[1]); vc=pltpu.make_async_copy(wv_ref,wv,qsem.at[2])
    def tile(s,j): return mbuf.at[s,:,pl.ds(pl.multiple_of(j*TW,TW) if not isinstance(j,int) else j*TW,TW)]
    def send(src,j,tgt,ss):
        return pltpu.make_async_remote_copy(src_ref=tile(src,j),dst_ref=tile(src,j),send_sem=ss,recv_sem=rsem.at[src,j],device_id=dev(tgt),device_id_type=MESH)
    def jcols(j): return pl.ds(pl.multiple_of(j*TW,TW),TW) if not isinstance(j,int) else pl.ds(j*TW,TW)
    def second(j,_):
        s=lax.rem(n1+j,NB)
        w2copy(j,s).wait()
        y=jnp.dot(inner[...],wbuf[s],preferred_element_type=F32)+b2_ref[jcols(j)].astype(F32).reshape(1,TW)
        mbuf[me,:,jcols(j)]=y.astype(BF)
        for a,tgt in enumerate((xn,yn,partner)): send(me,j,tgt,own_s.at[a,j]).start()
        @pl.when(j+NB<n2)
        def _(): w2copy(j+NB,s).start()
        return 0
    qc.start(); kc.start(); vc.start()
    lax.fori_loop(0,n2,second,0)
    for d in range(1,n):
        s=lax.rem(me+d,n)
        pltpu.make_async_remote_copy(src_ref=slots.at[s],dst_ref=slots.at[s],send_sem=slot_s.at[0],recv_sem=slot_r.at[s],device_id=dev(s),device_id_type=MESH).wait_recv()
    base=me*T
    def oh(s,_):
        sl=slots[s][0:1,:]
        tok=lax.broadcasted_iota(jnp.int32,(T,R),0)+base
        onehot[s]=jnp.where(tok==sl,1.0,0.0).astype(BF)
        return 0
    lax.fori_loop(0,n,oh,0)
    def place(s,j,firsttime=False):
        c=slice(j*TW,(j+1)*TW)
        p=jnp.dot(onehot[s],mbuf[s,:,c],preferred_element_type=F32)
        if firsttime: hacc[:,c]=p
        else: hacc[:,c]+=p
    for j in range(n2): place(me,j,True)
    fi=lax.broadcasted_iota(jnp.int32,(D//2,T),0)
    pos=jnp.where(fi<16,rp_ref[0:1,:],jnp.where(fi<40,rp_ref[1:2,:],rp_ref[2:3,:]))
    fr=jnp.zeros((D//2,D),F32); fj=lax.broadcasted_iota(jnp.int32,(D//2,D),0)
    for i in range(D//2): fr=jnp.where(fj==i,1000000.0**(-i/(D//2)),fr)
    ang=pos.astype(F32)*fr[:,0:1]
    cc=jnp.cos(ang); ss=jnp.sin(ang)
    cs[...]=jnp.concatenate([cc,cc],axis=0).T
    sn[...]=jnp.concatenate([-ss,ss],axis=0).T
    def arrive(s,j): send(s,j,partner,own_s.at[0,0]).wait_recv()
    fw=[]
    def forward(s,j,tgt,kind):
        c=send(s,j,tgt,fwd_s.at[kind,j]); c.start(); fw.append(c)
    for j in range(n2):
        arrive(xn,j)
        if j%2==0: forward(xn,j,yn,0)
        forward(xn,j,partner,1)
        arrive(yn,j)
        if j%2==1: forward(yn,j,xn,0)
        forward(yn,j,partner,2)
        arrive(partner,j)
        place(xn,j); place(yn,j); place(partner,j)
        if j>0:
            for s in (other(xn),other(yn)):
                arrive(s,j-1); place(s,j-1)
    for s in (other(xn),other(yn)):
        arrive(s,n2-1); place(s,n2-1)
    for j in range(n2):
        arrive(dg,j); forward(dg,j,partner,3); place(dg,j)
        if j>0: arrive(other(dg),j-1); place(other(dg),j-1)
    arrive(other(dg),n2-1); place(other(dg),n2-1)
    hit=onehot[0].astype(F32)
    for s in range(1,n): hit=hit+onehot[s].astype(F32)
    has=jnp.sum(hit,axis=1,keepdims=True)>0.5
    h0=jnp.where(has,hacc[...],emb_ref[...].astype(F32))
    h0_ref[...]=h0.astype(BF)
    a=(h0*lax.rsqrt(jnp.mean(h0*h0,axis=-1,keepdims=True)+1e-6)*na_ref[...].astype(F32).reshape(1,H)).astype(BF)
    qc.wait(); kc.wait(); vc.wait()
    def rope(x):
        return x*cs[...]+pltpu.roll(x,D//2,1)*sn[...]
    for i in range(H//TW):
        y=jnp.dot(a,wq[:,i*TW:(i+1)*TW],preferred_element_type=F32)+bq_ref[i*TW:(i+1)*TW].astype(F32).reshape(1,TW)
        for h in range(TW//D):
            q_ref[:,i*TW+h*D:i*TW+(h+1)*D]=rope(y[:,h*D:(h+1)*D]).astype(BF)
    y=jnp.dot(a,wk[...],preferred_element_type=F32)+bk_ref[...].astype(F32).reshape(1,-1)
    for h in range(wk.shape[1]//D):
        kt_ref[h*D:(h+1)*D,:]=rope(y[:,h*D:(h+1)*D]).T.astype(BF)
    v_ref[...]=(jnp.dot(a,wv[...],preferred_element_type=F32)+bv_ref[...].astype(F32).reshape(1,-1)).astype(BF)
    for d in range(1,n): slot_copy(d).wait_send()
    for j in range(n2):
        for a_,tgt in enumerate((xn,yn,partner)): send(me,j,tgt,own_s.at[a_,j]).wait_send()
    for c in fw: c.wait_send()
def front_call(pat,emb,slot,rope_pos,lw,lb,w1,b1,w2,b2,na,wq,bq,wk,bk,wv,bv,n=8):
    T,H=emb.shape; R=slot.shape[0]; K1=w1.shape[0]; V=pat.shape[1]; KV=wk.shape[1]
    vm=pl.BlockSpec(memory_space=pltpu.VMEM); hbm=pl.BlockSpec(memory_space=pl.ANY)
    n2=H//TW
    DS=pltpu.SemaphoreType.DMA
    return pl.pallas_call(functools.partial(front_body,n),
        out_shape=(jax.ShapeDtypeStruct((T,H),BF),jax.ShapeDtypeStruct((T,wq.shape[1]),BF),jax.ShapeDtypeStruct((KV,T),BF),jax.ShapeDtypeStruct((T,KV),BF)),
        in_specs=[vm,vm,vm,vm,vm,vm,hbm,vm,hbm,vm,vm,hbm,vm,hbm,vm,hbm,vm],
        out_specs=(vm,)*4,
        scratch_shapes=[pltpu.VMEM((V//D,128,D),F32),pltpu.VMEM((R,K1),BF),pltpu.VMEM((R,w1.shape[1]),BF),pltpu.VMEM((NB,K1,TW),BF),
            pltpu.VMEM((n,R,H),BF),pltpu.VMEM((n,8,R),jnp.int32),pltpu.VMEM((n,T,R),BF),pltpu.VMEM((T,H),F32),
            pltpu.VMEM(wq.shape,BF),pltpu.VMEM(wk.shape,BF),pltpu.VMEM(wv.shape,BF),pltpu.VMEM((T,D),F32),pltpu.VMEM((T,D),F32),
            DS((NB,)),DS((3,)),DS((n-1,)),DS((n,)),DS((3,n2)),DS((4,n2)),DS((n,n2))],
        compiler_params=pltpu.CompilerParams(collective_id=2,has_side_effects=True,vmem_limit_bytes=62*1024*1024),
        cost_estimate=pl.CostEstimate(flops=2*R*K1*(K1+H),bytes_accessed=2*K1*(K1+H),transcendentals=R*K1),
        name="front")(pat,emb,slot,rope_pos,lw,lb,w1,b1,w2,b2,na,wq,bq,wk,bk,wv,bv)
def mlp_body(h0_ref, at_ref, wo_ref, nm_ref, wg_ref, wu_ref, wd_ref, out_ref, h0, at, wo, wg, wu, wd, b, acc, sem):
    T,H=h0.shape; TF=wg.shape[2]; ns=wg_ref.shape[1]//TF
    first=[pltpu.make_async_copy(s,d,sem.at[2,i]) for i,(s,d) in enumerate(((at_ref,at),(wo_ref,wo),(h0_ref,h0)))]
    for c in first: c.start()
    cols=lambda i: pl.ds(pl.multiple_of(i*TF,TF),TF)
    def copies(i,k): return (pltpu.make_async_copy(wg_ref.at[:,cols(i)],wg.at[k],sem.at[k,0]),pltpu.make_async_copy(wu_ref.at[:,cols(i)],wu.at[k],sem.at[k,1]),pltpu.make_async_copy(wd_ref.at[cols(i),:],wd.at[k],sem.at[k,2]))
    for k in range(2):
        for c in copies(k,k): c.start()
    for c in first: c.wait()
    HT=T//2
    for r in range(2):
        rows=pl.ds(r*HT,HT)
        h1=(h0[rows,:].astype(F32)+jnp.dot(at[rows,:],wo[...],preferred_element_type=F32)).astype(BF).astype(F32)
        acc[rows,:]=h1
        b[rows,:]=(h1*lax.rsqrt(jnp.mean(h1*h1,axis=-1,keepdims=True)+1e-6)*nm_ref[...].astype(F32).reshape(1,H)).astype(BF)
    def step(i,_):
        k=lax.rem(i,2)
        for c in copies(i,k): c.wait()
        x=b[...]
        g=jnp.dot(x,wg[k],preferred_element_type=F32)
        u=jnp.dot(x,wu[k],preferred_element_type=F32)
        a=(g*jax.nn.sigmoid(g)*u).astype(BF)
        acc[...]+=jnp.dot(a,wd[k],preferred_element_type=F32)
        @pl.when(i+2<ns)
        def _():
            for c in copies(i+2,k): c.start()
        return 0
    lax.fori_loop(0,ns,step,0)
    out_ref[...]=acc[...].astype(BF)
def mlp_call(h0,at,wo,nm,wg,wu,wd,tf=1280):
    T,H=h0.shape; Fd=wg.shape[1]
    hbm=pl.BlockSpec(memory_space=pl.ANY); vm=pl.BlockSpec(memory_space=pltpu.VMEM)
    V=pltpu.VMEM
    return pl.pallas_call(mlp_body,
        out_shape=jax.ShapeDtypeStruct((T,H),BF),
        in_specs=[hbm,hbm,hbm,vm,hbm,hbm,hbm],
        out_specs=vm,
        scratch_shapes=[V((T,H),BF),V(at.shape,BF),V(wo.shape,BF),V((2,H,tf),BF),V((2,H,tf),BF),V((2,tf,H),BF),V((T,H),BF),V((T,H),F32),pltpu.SemaphoreType.DMA((3,3))],
        compiler_params=pltpu.CompilerParams(vmem_limit_bytes=60*1024*1024),
        cost_estimate=pl.CostEstimate(flops=2*T*H*(H+3*Fd),bytes_accessed=2*H*(H+3*Fd),transcendentals=T*Fd),
        name="mlp")(h0,at,wo,nm,wg,wu,wd)


def solution(mesh):
    group_size = mesh.shape['sp']
    row_spec = P(('dp', 'sp'), None)

    def local_step(patches, embeds, dest_slot, rope_pos, cu_doc, ln_w, ln_b, w_one, b_one, w_two, b_two, norm_attn, w_q, b_q, w_k, b_k, w_v, b_v, w_o, norm_mlp, w_gate, w_up, w_down):
        h_zero, q, k, v = front_call(patches, embeds, dest_slot, rope_pos, ln_w, ln_b, w_one, b_one, w_two, b_two, norm_attn, w_q, b_q, w_k, b_k, w_v, b_v, group_size)
        attn_out = attn_call(cu_doc, q, k, v, group_size)
        return mlp_call(h_zero, attn_out, w_o, norm_mlp, w_gate, w_up, w_down)

    in_specs = (row_spec, row_spec, P(('dp', 'sp')), P(None, ('dp', 'sp')), P('dp')) + (P(),) * 18
    return jax.shard_map(local_step, mesh=mesh, in_specs=in_specs, out_specs=row_spec, check_vma=False)
```

```python
import functools
import jax
import jax.numpy as jnp
from jax import lax
from jax.experimental import pallas as pl
from jax.experimental.pallas import tpu as pltpu
from jax.sharding import PartitionSpec as P

BF = jnp.bfloat16
F32 = jnp.float32
MESH = pl.DeviceIdType.MESH
D = 128
SC=D**-0.5*1.4426950408889634
def attn_body(n, nh, nkv, cu_ref, q_ref, kt_ref, v_ref, o_ref, qa, kb, vb, acc, mx, ls, sb, pb, ssem, rsem, fsem):
    T=q_ref.shape[0]; grp=nh//nkv
    ncut=cu_ref.shape[0]-2
    me=lax.axis_index('sp'); chip=me//2; core=lax.rem(me,2); partner=chip*2+1-core
    dev=lambda i: {'sp':i}
    bar=pltpu.get_barrier_semaphore()
    for d in range(1,n):
        pl.semaphore_signal(bar,inc=1,device_id=dev(lax.rem(me+d,n)),device_id_type=MESH)
    lane=lax.broadcasted_iota(jnp.int32,(T,D),1); rowq=lax.broadcasted_iota(jnp.int32,(T,D),0)+me*T
    tail=jnp.zeros((T,D),F32)
    for d in range(ncut):
        tail=jnp.where((lane==d)&(rowq>=cu_ref[1+d]),-1e30,tail)
    tail=tail.astype(BF)
    pl.semaphore_wait(bar,n-1)
    def rcopy(what,src_s,g,tgt,sem_s,sem_r,loc=False):
        if what==0:
            src=kt_ref.at[pl.ds(g*D,D),:] if loc else kb.at[src_s,g,pl.ds(0,D),:]
            dst=kb.at[src_s,g,pl.ds(0,D),:]
        else:
            src=v_ref.at[:,pl.ds(g*D,D)] if loc else vb.at[src_s,g]
            dst=vb.at[src_s,g]
        return pltpu.make_async_remote_copy(src_ref=src,dst_ref=dst,send_sem=sem_s,recv_sem=sem_r,device_id=dev(tgt),device_id_type=MESH)
    def my_send(dc,g,w):
        tgt=partner if dc==0 else me+2*dc
        return rcopy(w,me,g,tgt,ssem.at[dc,g,w],rsem.at[me,g,w],loc=True)
    def send_cond(dc):
        return (core==0) if dc==0 else (me+2*dc<n)
    for dc in range(n//2):
        @pl.when(send_cond(dc))
        def _(dc=dc):
            for g in range(nkv):
                for w in range(2): my_send(dc,g,w).start()
    def fill(s,_):
        krow=lax.broadcasted_iota(jnp.int32,(D,T),0); kpos=lax.broadcasted_iota(jnp.int32,(D,T),1)+s*T
        kt=jnp.zeros((D,T),F32)
        for d in range(ncut):
            kt=jnp.where((krow==d)&(kpos<cu_ref[1+d]),1.0,kt)
        kt=kt.astype(BF)
        for g in range(nkv): kb[s,g,pl.ds(D,D),:]=kt
        return 0
    lax.fori_loop(0,me+1,fill,0)
    for h in range(nh):
        qa[h,:,:D]=q_ref[:,h*D:(h+1)*D]
        qa[h,:,D:]=tail
    for g in range(nkv):
        kb[me,g,pl.ds(0,D),:]=kt_ref[g*D:(g+1)*D,:]
        vb[me,g]=v_ref[:,g*D:(g+1)*D]
    def qk(h,s,g): return jnp.dot(qa[h],kb[s,g],preferred_element_type=F32)
    def soft(h,sc):
        mp=mx[h]
        m=jnp.maximum(mp,jnp.max(sc,axis=1,keepdims=True)*SC)
        al=jnp.exp2(mp-m)
        l=ls[h]*al; ps=[]
        for j in range(T//D):
            p=jnp.exp2(sc[:,j*D:(j+1)*D]*SC-m); l=l+p; ps.append(p.astype(BF))
        mx[h]=m; ls[h]=l
        return jnp.concatenate(ps,axis=1),al
    def pv(h,s,g,p,al):
        acc[h]=acc[h]*al+jnp.dot(p,vb[s,g],preferred_element_type=F32)
    def soft_own(h,sc):
        qi=lax.broadcasted_iota(jnp.int32,(T,T),0); ki=lax.broadcasted_iota(jnp.int32,(T,T),1)
        sc=jnp.where(ki<=qi,sc,-1e30)
        m=jnp.broadcast_to(jnp.max(sc,axis=1,keepdims=True)*SC,(T,D))
        l=None; ps=[]
        for j in range(T//D):
            p=jnp.exp2(sc[:,j*D:(j+1)*D]*SC-m); l=p if l is None else l+p
            ps.append(p.astype(BF))
        mx[h]=m; ls[h]=l
        return jnp.concatenate(ps,axis=1)
    def pv_own(h,g,p): acc[h]=jnp.dot(p,vb[me,g],preferred_element_type=F32)
    def own(g,_):
        h0=g*grp
        sb[0]=qk(h0,me,g)
        for hh in range(grp):
            h=h0+hh
            if hh+1<grp: sb[(hh+1)%2]=qk(h+1,me,g)
            if hh>0: pv_own(h-1,g,pb[(hh-1)%2])
            pb[hh%2]=soft_own(h,sb[hh%2])
        pv_own(h0+grp-1,g,pb[(grp-1)%2])
        return 0
    lax.fori_loop(0,nkv,own,0)
    def wait_recv(s,g):
        for w in range(2): rcopy(w,s,g,partner,fsem.at[0,g,w],rsem.at[s,g,w]).wait_recv()
    def fwd(s,g,w,dc): return rcopy(w,s,g,partner,fsem.at[dc,g,w],rsem.at[s,g,w])
    def shard_step(i,_):
        j=i-core
        dc=jnp.where(j<0,0,j//2+1)
        direct=(j>=0)&(lax.rem(j+2,2)==0)
        s=jnp.where(j<0,partner,(chip-dc)*2+jnp.where(direct,core,1-core))
        def per_g(g,_):
            wait_recv(s,g)
            @pl.when(direct)
            def _():
                for w in range(2): fwd(s,g,w,dc).start()
            sb[0]=qk(g*grp,s,g); pal=None
            for hh in range(grp):
                h=g*grp+hh
                if hh>0: pv(h-1,s,g,pb[(hh-1)%2],pal)
                if hh+1<grp: sb[(hh+1)%2]=qk(h+1,s,g)
                p,pal=soft(h,sb[hh%2])
                pb[hh%2]=p
            pv(g*grp+grp-1,s,g,pb[(grp-1)%2],pal)
            return 0
        lax.fori_loop(0,nkv,per_g,0)
        return 0
    lax.fori_loop(0,2*chip+core,shard_step,0)
    for h in range(nh):
        o_ref[:,h*D:(h+1)*D]=(acc[h]/jnp.sum(ls[h],axis=1,keepdims=True)).astype(BF)
    for dc in range(n//2):
        @pl.when(send_cond(dc))
        def _(dc=dc):
            for g in range(nkv):
                for w in range(2): my_send(dc,g,w).wait_send()
    for dc in range(1,n//2):
        @pl.when(chip-dc>=0)
        def _(dc=dc):
            s=(chip-dc)*2+core
            for g in range(nkv):
                for w in range(2): fwd(s,g,w,dc).wait_send()
def attn_call(cu,q,kt,v,n=8):
    T,HQ=q.shape; nh=HQ//D; nkv=kt.shape[0]//D
    vm=pl.BlockSpec(memory_space=pltpu.VMEM)
    return pl.pallas_call(functools.partial(attn_body,n,nh,nkv),
        out_shape=jax.ShapeDtypeStruct((T,HQ),BF),
        in_specs=[pl.BlockSpec(memory_space=pltpu.SMEM),vm,vm,vm],
        out_specs=vm,
        scratch_shapes=[pltpu.VMEM((nh,T,2*D),BF),pltpu.VMEM((n,nkv,2*D,T),BF),pltpu.VMEM((n,nkv,T,D),BF),
            pltpu.VMEM((nh,T,D),F32),pltpu.VMEM((nh,T,D),F32),pltpu.VMEM((nh,T,D),F32),
            pltpu.VMEM((2,T,T),F32),pltpu.VMEM((2,T,T),BF),
            pltpu.SemaphoreType.DMA((n//2,nkv,2)),pltpu.SemaphoreType.DMA((n,nkv,2)),pltpu.SemaphoreType.DMA((n//2,nkv,2))],
        compiler_params=pltpu.CompilerParams(collective_id=1,has_side_effects=True,vmem_limit_bytes=56*1024*1024),
        cost_estimate=pl.CostEstimate(flops=4*T*T*n*HQ,bytes_accessed=4*T*HQ,transcendentals=T*T*n*nh),
        name="attn")(cu,q,kt,v)
TW=256
NB=5
def front_body(n, pat_ref, emb_ref, slot_ref, rp_ref, lw_ref, lb_ref, w1_ref, b1_ref, w2_ref, b2_ref, na_ref, wq_ref, bq_ref, wk_ref, bk_ref, wv_ref, bv_ref,
               h0_ref, q_ref, kt_ref, v_ref,
               zf, z, inner, wbuf, mbuf, slots, onehot, hacc, wq, wk, wv,
               cs, sn, h0b, qb, osem, wsem, qsem, slot_s, slot_r, own_s, fwd_s, rsem):
    R=mbuf.shape[1]; T=emb_ref.shape[0]; V=pat_ref.shape[1]; K1=w1_ref.shape[0]; H=w2_ref.shape[1]
    n1=w1_ref.shape[1]//TW; n2=H//TW
    me=lax.axis_index('sp'); chip=me//2; core=lax.rem(me,2)
    partner=chip*2+1-core
    cx=lax.rem(chip,2); cy=chip//2
    xn=(cy*2+1-cx)*2+core; yn=((1-cy)*2+cx)*2+core; dg=((1-cy)*2+1-cx)*2+core
    other=lambda i: i+1-2*core
    dev=lambda i: {'sp':i}
    bar=pltpu.get_barrier_semaphore()
    for d in range(1,n):
        pl.semaphore_signal(bar,inc=1,device_id=dev(lax.rem(me+d,n)),device_id_type=MESH)
    def w1copy(t,s): return pltpu.make_async_copy(w1_ref.at[:,pl.ds(pl.multiple_of(t*TW,TW),TW)],wbuf.at[s],wsem.at[s])
    def w2copy(t,s): return pltpu.make_async_copy(w2_ref.at[:,pl.ds(pl.multiple_of(t*TW,TW),TW)],wbuf.at[s],wsem.at[s])
    for t in range(NB): w1copy(t,t).start()
    slots[me]=jnp.broadcast_to(slot_ref[...].reshape(1,R),(8,R))
    lw=lw_ref[...].astype(F32).reshape(1,V); lb=lb_ref[...].astype(F32).reshape(1,V)
    CH=128
    def ln(i,_):
        x=pat_ref[pl.ds(pl.multiple_of(i*CH,CH),CH),:].astype(F32)
        c=x-jnp.mean(x,axis=-1,keepdims=True)
        var=jnp.mean(c*c,axis=-1,keepdims=True)
        y=c*lax.rsqrt(var+1e-6)*lw+lb
        for p in range(V//D): zf[p]=y[:,p*D:(p+1)*D]
        for j in range(4):
            for p in range(V//D):
                z[pl.ds(pl.multiple_of(i*(CH//4),CH//4),CH//4),j*V+p*D:j*V+(p+1)*D]=zf[p,pl.ds(j,CH//4,stride=4),:].astype(BF)
        return 0
    lax.fori_loop(0,pat_ref.shape[0]//CH,ln,0)
    pl.semaphore_wait(bar,n-1)
    def slot_copy(d):
        return pltpu.make_async_remote_copy(src_ref=slots.at[me],dst_ref=slots.at[me],send_sem=slot_s.at[d-1],recv_sem=slot_r.at[me],device_id=dev(lax.rem(me+d,n)),device_id_type=MESH)
    for d in range(1,n): slot_copy(d).start()
    def first(i,_):
        s=lax.rem(i,NB)
        w1copy(i,s).wait()
        y=jnp.dot(z[...],wbuf[s],preferred_element_type=F32)
        cols=pl.ds(pl.multiple_of(i*TW,TW),TW)
        y=y+b1_ref[cols].astype(F32).reshape(1,TW)
        inner[:,cols]=(0.5*y*(1.0+lax.erf(y*0.7071067811865476))).astype(BF)
        @pl.when(i+NB<n1)
        def _(): w1copy(i+NB,s).start()
        @pl.when(i+NB>=n1)
        def _(): w2copy(i+NB-n1,s).start()
        return 0
    lax.fori_loop(0,n1,first,0)
    qc=pltpu.make_async_copy(wq_ref,wq,qsem.at[0]); kc=pltpu.make_async_copy(wk_ref,wk,qsem.at[1]); vc=pltpu.make_async_copy(wv_ref,wv,qsem.at[2])
    def tile(s,j): return mbuf.at[s,:,pl.ds(pl.multiple_of(j*TW,TW) if not isinstance(j,int) else j*TW,TW)]
    def send(src,j,tgt,ss):
        return pltpu.make_async_remote_copy(src_ref=tile(src,j),dst_ref=tile(src,j),send_sem=ss,recv_sem=rsem.at[src,j],device_id=dev(tgt),device_id_type=MESH)
    def jcols(j): return pl.ds(pl.multiple_of(j*TW,TW),TW) if not isinstance(j,int) else pl.ds(j*TW,TW)
    def second(j,_):
        s=lax.rem(n1+j,NB)
        w2copy(j,s).wait()
        y=jnp.dot(inner[...],wbuf[s],preferred_element_type=F32)+b2_ref[jcols(j)].astype(F32).reshape(1,TW)
        mbuf[me,:,jcols(j)]=y.astype(BF)
        for a,tgt in enumerate((xn,yn,partner)): send(me,j,tgt,own_s.at[a,j]).start()
        @pl.when(j+NB<n2)
        def _(): w2copy(j+NB,s).start()
        return 0
    qc.start(); kc.start(); vc.start()
    lax.fori_loop(0,n2,second,0)
    for d in range(1,n):
        s=lax.rem(me+d,n)
        pltpu.make_async_remote_copy(src_ref=slots.at[s],dst_ref=slots.at[s],send_sem=slot_s.at[0],recv_sem=slot_r.at[s],device_id=dev(s),device_id_type=MESH).wait_recv()
    base=me*T
    def oh(s,_):
        sl=slots[s][0:1,:]
        tok=lax.broadcasted_iota(jnp.int32,(T,R),0)+base
        onehot[s]=jnp.where(tok==sl,1.0,0.0).astype(BF)
        return 0
    lax.fori_loop(0,n,oh,0)
    def place(s,j):
        c=slice(j*TW,(j+1)*TW)
        p=jnp.dot(onehot[s],mbuf[s,:,c],preferred_element_type=F32)
        hacc[:,c]+=p
    hit=onehot[0].astype(F32)
    for s in range(1,n): hit=hit+onehot[s].astype(F32)
    has=jnp.sum(hit,axis=1,keepdims=True)>0.5
    hacc[...]=jnp.where(has,0.0,emb_ref[...].astype(F32))
    for j in range(n2): place(me,j)
    fi=lax.broadcasted_iota(jnp.int32,(D//2,T),0)
    pos=jnp.where(fi<16,rp_ref[0:1,:],jnp.where(fi<40,rp_ref[1:2,:],rp_ref[2:3,:]))
    fr=jnp.zeros((D//2,D),F32); fj=lax.broadcasted_iota(jnp.int32,(D//2,D),0)
    for i in range(D//2): fr=jnp.where(fj==i,1000000.0**(-i/(D//2)),fr)
    ang=pos.astype(F32)*fr[:,0:1]
    cc=jnp.cos(ang); ss=jnp.sin(ang)
    cs[...]=jnp.concatenate([cc,cc],axis=0).T
    sn[...]=jnp.concatenate([-ss,ss],axis=0).T
    def arrive(s,j): send(s,j,partner,own_s.at[0,0]).wait_recv()
    fw=[]
    def forward(s,j,tgt,kind):
        c=send(s,j,tgt,fwd_s.at[kind,j]); c.start(); fw.append(c)
    for j in range(n2):
        arrive(xn,j)
        if j%2==0: forward(xn,j,yn,0)
        forward(xn,j,partner,1)
        arrive(yn,j)
        if j%2==1: forward(yn,j,xn,0)
        forward(yn,j,partner,2)
        arrive(partner,j)
        place(xn,j); place(yn,j); place(partner,j)
        if j>0:
            for s in (other(xn),other(yn)):
                arrive(s,j-1); place(s,j-1)
    for s in (other(xn),other(yn)):
        arrive(s,n2-1); place(s,n2-1)
    for j in range(n2):
        arrive(dg,j); forward(dg,j,partner,3); place(dg,j)
        if j>0: arrive(other(dg),j-1); place(other(dg),j-1)
    arrive(other(dg),n2-1); place(other(dg),n2-1)
    h0=hacc[...]
    h0b[...]=h0.astype(BF)
    outs=[pltpu.make_async_copy(h0b,h0_ref,osem.at[0])]; outs[0].start()
    a=(h0*lax.rsqrt(jnp.mean(h0*h0,axis=-1,keepdims=True)+1e-6)*na_ref[...].astype(F32).reshape(1,H)).astype(BF)
    qc.wait(); kc.wait(); vc.wait()
    def rope(x):
        return x*cs[...]+pltpu.roll(x,D//2,1)*sn[...]
    for i in range(H//TW):
        y=jnp.dot(a,wq[:,i*TW:(i+1)*TW],preferred_element_type=F32)+bq_ref[i*TW:(i+1)*TW].astype(F32).reshape(1,TW)
        for h in range(TW//D):
            qb[:,i*TW+h*D:i*TW+(h+1)*D]=rope(y[:,h*D:(h+1)*D]).astype(BF)
        o=pltpu.make_async_copy(qb.at[:,pl.ds(i*TW,TW)],q_ref.at[:,pl.ds(i*TW,TW)],osem.at[1+i]); o.start(); outs.append(o)
    y=jnp.dot(a,wk[...],preferred_element_type=F32)+bk_ref[...].astype(F32).reshape(1,-1)
    for h in range(wk.shape[1]//D):
        kt_ref[h*D:(h+1)*D,:]=rope(y[:,h*D:(h+1)*D]).T.astype(BF)
    v_ref[...]=(jnp.dot(a,wv[...],preferred_element_type=F32)+bv_ref[...].astype(F32).reshape(1,-1)).astype(BF)
    for o in outs: o.wait()
    for d in range(1,n): slot_copy(d).wait_send()
    for j in range(n2):
        for a_,tgt in enumerate((xn,yn,partner)): send(me,j,tgt,own_s.at[a_,j]).wait_send()
    for c in fw: c.wait_send()
def front_call(pat,emb,slot,rope_pos,lw,lb,w1,b1,w2,b2,na,wq,bq,wk,bk,wv,bv,n=8):
    T,H=emb.shape; R=slot.shape[0]; K1=w1.shape[0]; V=pat.shape[1]; KV=wk.shape[1]
    vm=pl.BlockSpec(memory_space=pltpu.VMEM); hbm=pl.BlockSpec(memory_space=pl.ANY)
    n2=H//TW
    DS=pltpu.SemaphoreType.DMA
    return pl.pallas_call(functools.partial(front_body,n),
        out_shape=(jax.ShapeDtypeStruct((T,H),BF),jax.ShapeDtypeStruct((T,wq.shape[1]),BF),jax.ShapeDtypeStruct((KV,T),BF),jax.ShapeDtypeStruct((T,KV),BF)),
        in_specs=[vm,vm,vm,vm,vm,vm,hbm,vm,hbm,vm,vm,hbm,vm,hbm,vm,hbm,vm],
        out_specs=(hbm,hbm,vm,vm),
        scratch_shapes=[pltpu.VMEM((V//D,128,D),F32),pltpu.VMEM((R,K1),BF),pltpu.VMEM((R,w1.shape[1]),BF),pltpu.VMEM((NB,K1,TW),BF),
            pltpu.VMEM((n,R,H),BF),pltpu.VMEM((n,8,R),jnp.int32),pltpu.VMEM((n,T,R),BF),pltpu.VMEM((T,H),F32),
            pltpu.VMEM(wq.shape,BF),pltpu.VMEM(wk.shape,BF),pltpu.VMEM(wv.shape,BF),pltpu.VMEM((T,D),F32),pltpu.VMEM((T,D),F32),pltpu.VMEM((T,H),BF),pltpu.VMEM((T,wq.shape[1]),BF),DS((1+n2,)),
            DS((NB,)),DS((3,)),DS((n-1,)),DS((n,)),DS((3,n2)),DS((4,n2)),DS((n,n2))],
        compiler_params=pltpu.CompilerParams(collective_id=2,has_side_effects=True,vmem_limit_bytes=62*1024*1024),
        cost_estimate=pl.CostEstimate(flops=2*R*K1*(K1+H),bytes_accessed=2*K1*(K1+H),transcendentals=R*K1),
        name="front")(pat,emb,slot,rope_pos,lw,lb,w1,b1,w2,b2,na,wq,bq,wk,bk,wv,bv)
def mlp_body(h0_ref, at_ref, wo_ref, nm_ref, wg_ref, wu_ref, wd_ref, out_ref, h0, at, wo, wg, wu, wd, b, acc, sem):
    T,H=h0.shape; TF=wg.shape[2]; ns=wg_ref.shape[1]//TF
    first=[pltpu.make_async_copy(s,d,sem.at[2,i]) for i,(s,d) in enumerate(((at_ref,at),(wo_ref,wo),(h0_ref,h0)))]
    for c in first: c.start()
    cols=lambda i: pl.ds(pl.multiple_of(i*TF,TF),TF)
    def copies(i,k): return (pltpu.make_async_copy(wg_ref.at[:,cols(i)],wg.at[k],sem.at[k,0]),pltpu.make_async_copy(wu_ref.at[:,cols(i)],wu.at[k],sem.at[k,1]),pltpu.make_async_copy(wd_ref.at[cols(i),:],wd.at[k],sem.at[k,2]))
    for k in range(2):
        for c in copies(k,k): c.start()
    for c in first: c.wait()
    HT=T//2
    for r in range(2):
        rows=pl.ds(r*HT,HT)
        h1=(h0[rows,:].astype(F32)+jnp.dot(at[rows,:],wo[...],preferred_element_type=F32)).astype(BF).astype(F32)
        acc[rows,:]=h1
        b[rows,:]=(h1*lax.rsqrt(jnp.mean(h1*h1,axis=-1,keepdims=True)+1e-6)*nm_ref[...].astype(F32).reshape(1,H)).astype(BF)
    def step(i,_):
        k=lax.rem(i,2)
        for c in copies(i,k): c.wait()
        x=b[...]
        g=jnp.dot(x,wg[k],preferred_element_type=F32)
        u=jnp.dot(x,wu[k],preferred_element_type=F32)
        a=(g*jax.nn.sigmoid(g)*u).astype(BF)
        acc[...]+=jnp.dot(a,wd[k],preferred_element_type=F32)
        @pl.when(i+2<ns)
        def _():
            for c in copies(i+2,k): c.start()
        return 0
    lax.fori_loop(0,ns,step,0)
    out_ref[...]=acc[...].astype(BF)
def mlp_call(h0,at,wo,nm,wg,wu,wd,tf=1280):
    T,H=h0.shape; Fd=wg.shape[1]
    hbm=pl.BlockSpec(memory_space=pl.ANY); vm=pl.BlockSpec(memory_space=pltpu.VMEM)
    V=pltpu.VMEM
    return pl.pallas_call(mlp_body,
        out_shape=jax.ShapeDtypeStruct((T,H),BF),
        in_specs=[hbm,hbm,hbm,vm,hbm,hbm,hbm],
        out_specs=vm,
        scratch_shapes=[V((T,H),BF),V(at.shape,BF),V(wo.shape,BF),V((2,H,tf),BF),V((2,H,tf),BF),V((2,tf,H),BF),V((T,H),BF),V((T,H),F32),pltpu.SemaphoreType.DMA((3,3))],
        compiler_params=pltpu.CompilerParams(vmem_limit_bytes=60*1024*1024),
        cost_estimate=pl.CostEstimate(flops=2*T*H*(H+3*Fd),bytes_accessed=2*H*(H+3*Fd),transcendentals=T*Fd),
        name="mlp")(h0,at,wo,nm,wg,wu,wd)


def solution(mesh):
    group_size = mesh.shape['sp']
    row_spec = P(('dp', 'sp'), None)

    def local_step(patches, embeds, dest_slot, rope_pos, cu_doc, ln_w, ln_b, w_one, b_one, w_two, b_two, norm_attn, w_q, b_q, w_k, b_k, w_v, b_v, w_o, norm_mlp, w_gate, w_up, w_down):
        h_zero, q, k, v = front_call(patches, embeds, dest_slot, rope_pos, ln_w, ln_b, w_one, b_one, w_two, b_two, norm_attn, w_q, b_q, w_k, b_k, w_v, b_v, group_size)
        attn_out = attn_call(cu_doc, q, k, v, group_size)
        return mlp_call(h_zero, attn_out, w_o, norm_mlp, w_gate, w_up, w_down)

    in_specs = (row_spec, row_spec, P(('dp', 'sp')), P(None, ('dp', 'sp')), P('dp')) + (P(),) * 18
    return jax.shard_map(local_step, mesh=mesh, in_specs=in_specs, out_specs=row_spec, check_vma=False)
```
